512 devices in a mesh: parts: 2 (over y), slab: 32 (over z), orb: 4 (over x), pen: 2 (over core).
Axes of the slice: x: 4, y: 2, z: 32, core: 2. Of those that a mesh axis runs over, the one named last changes fastest.
The devices are a block of a 4x8x32 slice.
Arguments:
- orbitals: float32 [128, 128, 8, 256], P(('parts', 'orb'), 'slab', 'pen'), parts along dimension 0, may hold values from -7.6 to 7.6
- energies: float32 [128], P(('parts', 'orb')), parts along dimension 0, may hold values from -1 to 0.5
- frequency: float32 [2], P('parts'), parts along dimension 0, may hold values from 0.5 to 2
- local_potential: float32 [128, 8, 256], P('slab', 'pen'), may hold values from -1 to 1
- perturbation: float32 [128, 8, 256], P('slab', 'pen'), may hold values from 0.5 to 1.5
- projectors: float32 [128, 8, 256], P(None, 'pen'), may hold values from -0.0625 to 0.0625
- profiles: float32 [128, 5], replicated, may hold values from 0.5 to 2
- couplings: float32 [128], replicated, may hold values from 4 to 12
- atom_planes: int32 [128], replicated, may hold values from 0 to 127
Outputs:
- response_real: float32 [128, 128, 8, 256], P(('parts', 'orb'), 'slab', 'pen'), parts along dimension 0
- density: float32 [256, 8, 256], P(('parts', 'slab'), 'pen'), parts along dimension 0
The draws below stay inside these ranges and needn't reach their ends.
There are 2 independent parts, one for each index of `parts`. The reference program is written for one: setup_inputs(seed, part) draws one part's arguments, and reference() takes and returns one part's arrays. A program takes and returns all parts, laid end to end along the dimension named above; an argument that names none is the same for every part. Nothing has to cross between parts.
Inputs may be any that keep to these rules, and one draw needn't show every extreme that they name: Projector a covers the planes (atom_planes[a] + d) mod 128 of the first dimension for d < 5.
All inputs are finite; a program needn't handle non-finite values.
Results may differ from the reference program's by a relative error of at most 0.0003.
Values sent between devices are 32-bit elements; how exact they have to be, the bound alone decides.
No kernel may reach another device: no remote copies, remote signals or barrier semaphores. Data moves between devices by JAX's collectives and lax.ppermute only.
A program may use at most 64 MiB of HBM per device.

```python
import math
import jax
import jax.numpy as jnp
from jax import lax

NOCC = 64
NPROJ = 128
PSPAN = 5
ITERS = 2
NX = 256
NZ = 128
NY = 8
NCELL = 262144


def draw_orbitals(key, part):
    key_own = jax.random.fold_in(key, 11)
    key_common = jax.random.fold_in(key, 12)
    key_mix = jax.random.fold_in(key, 13)
    own_part = jnp.clip(jax.random.normal(key_own, (NOCC, NZ, NY, NX), jnp.float32), -4.0, 4.0)
    common_part = jnp.clip(jax.random.normal(key_common, (NZ, NY, NX), jnp.float32), -4.0, 4.0)
    mixing = jax.random.uniform(key_mix, (NOCC,), jnp.float32, 0.3, 0.7)
    return own_part + mixing[:, None, None, None] * common_part[None]


def potential_field(key):
    key_size = jax.random.fold_in(key, 21)
    key_sign = jax.random.fold_in(key, 22)
    magnitude = jax.random.uniform(key_size, (NZ, NY, NX), jnp.float32, 0.3, 1.0)
    signs = jnp.where(jax.random.bernoulli(key_sign, 0.5, (NZ, NY, NX)), 1.0, -1.0).astype(jnp.float32)
    return magnitude * signs


def draw_local_potential(key, part):
    return potential_field(key)


def draw_perturbation(key, part):
    potential = potential_field(key)
    noise = jax.random.uniform(jax.random.fold_in(key, 23), (NZ, NY, NX), jnp.float32, -1.0, 1.0)
    return jnp.clip(1.0 + 0.5 * potential + 0.04 * noise, 0.5, 1.5)


def with_ends(entries, key, smallest, largest):
    dims = entries.shape
    index_at = [jax.random.randint(jax.random.fold_in(key, axis), (), 0, dims[axis]) for axis in range(len(dims))]
    entries = entries.at[tuple(index_at)].set(smallest)
    longest = dims.index(max(dims))
    index_at[longest] = (index_at[longest] + 1) % dims[longest]
    return entries.at[tuple(index_at)].set(largest)


def level_of(own_key, shape, cuts, smallest, high):
    factor_of, own = 1.0, jax.random.fold_in(own_key, 6)
    for position, blocks in cuts:
        steps = jnp.exp(jax.random.uniform(jax.random.fold_in(own, position), (blocks,), jnp.float32, smallest / len(cuts), high / len(cuts)))
        factor_of = factor_of * jnp.repeat(steps, shape[position] // blocks).reshape([-1 if axis == position else 1 for axis in range(len(shape))])
    return factor_of


def gaussian(rng, extent, scale, most, shards=(), kind=jnp.bfloat16):
    drawn = jax.random.normal(rng, extent, jnp.float32) * scale
    if len(shards) > 0:
        drawn = level_of(rng, extent, shards, -0.22, 0.18) * drawn
    return jnp.clip(drawn, min=-most, max=most).astype(kind)


def setup_inputs(seed: int = 0, part: int = 0) -> dict:
    key_list = jax.random.split(jax.random.key(seed), 10)
    part_keys = jax.random.split(jax.random.fold_in(key_list[9], part), 10)
    orbitals = draw_orbitals(jax.random.fold_in(jax.random.fold_in(key_list[9], part), 71), part)
    energies = jnp.clip(-1.0 + 1.5 * jax.random.uniform(part_keys[1], (NOCC,), jnp.float32) ** level_of(part_keys[1], (NOCC,), ((0, 4),), -0.2, 0.2), -1.0, 0.5)
    frequency = jnp.clip(jnp.exp(jax.random.uniform(part_keys[2], (1,), jnp.float32, math.log(0.5), math.log(2.0))), 0.5, 2.0)
    local_potential = draw_local_potential(jax.random.fold_in(key_list[9], 71), part)
    perturbation = draw_perturbation(jax.random.fold_in(key_list[9], 71), part)
    projectors = gaussian(key_list[5], (NPROJ, NY, NX), (PSPAN * NY * NX) ** -0.5, 0.0625, ((1, 2),), jnp.float32)
    profiles = jnp.clip(jax.random.uniform(key_list[6], (NPROJ, PSPAN), jnp.float32, 0.5, 2.0), 0.5, 2.0)
    couplings = jnp.clip(jax.random.uniform(key_list[7], (NPROJ,), jnp.float32, 4.0, 12.0), 4.0, 12.0)
    atom_planes = with_ends(jax.random.randint(key_list[8], (NPROJ,), 0, NZ), jax.random.fold_in(key_list[8], 1), 0, NZ - 1).astype(jnp.int32)
    return {"orbitals": orbitals, "energies": energies, "frequency": frequency, "local_potential": local_potential, "perturbation": perturbation, "projectors": projectors, "profiles": profiles, "couplings": couplings, "atom_planes": atom_planes}


kinetic_scale = 0.125
highest = lax.Precision.HIGHEST

def kinetic(values):
    beside_all = jnp.roll(values, 1, 1) + jnp.roll(values, -1, 1)
    beside_all = beside_all + jnp.roll(values, 1, 2) + jnp.roll(values, -1, 2)
    beside_all = beside_all + jnp.roll(values, 1, 3) + jnp.roll(values, -1, 3)
    return kinetic_scale * (6.0 * values - beside_all)

def plane_weights(atom_planes, profiles, planes):
    span_size = profiles.shape[1]
    covered = (atom_planes[:, None] + jnp.arange(span_size, dtype=jnp.int32)[None, :]) % NZ
    matches = (covered[:, :, None] == planes[None, None, :]).astype(jnp.float32)
    return jnp.sum(profiles[:, :, None] * matches, axis=1)

def shifted(values, local_potential, projectors, weights, couplings, energies):
    inner_sums = jnp.einsum('ayx,izyx->aiz', projectors, values, precision=highest)
    expansion = couplings[:, None] * jnp.einsum('aiz,az->ai', inner_sums, weights, precision=highest)
    spread = weights[:, None, :] * expansion[:, :, None]
    nonlocal_term = jnp.einsum('aiz,ayx->izyx', spread, projectors, precision=highest)
    return kinetic(values) + local_potential[None] * values + nonlocal_term - energies[:, None, None, None] * values

def remove(values, orbitals, factor):
    correlation = jnp.einsum('jzyx,izyx->ji', orbitals, values, precision=highest) / NCELL
    expansion = jax.scipy.linalg.cho_solve((factor, True), correlation)
    return values - jnp.einsum('ji,jzyx->izyx', expansion, orbitals, precision=highest)

def reference(orbitals, energies, frequency, local_potential, perturbation, projectors, profiles, couplings, atom_planes):
    weights = plane_weights(atom_planes, profiles, jnp.arange(NZ, dtype=jnp.int32))
    gram = jnp.einsum('jzyx,kzyx->jk', orbitals, orbitals, precision=highest) / NCELL
    factor = jnp.linalg.cholesky(gram)
    freq_square = frequency[0] * frequency[0]

    def apply_shift(values):
        return shifted(values, local_potential, projectors, weights, couplings, energies)
    residual = -remove(perturbation[None] * orbitals, orbitals, factor)
    direction = residual
    solution = jnp.zeros_like(residual)
    norm_now = jnp.sum(residual * residual, axis=(1, 2, 3))
    for iteration in range(ITERS):
        inner_field = remove(direction, orbitals, factor)
        first_half = apply_shift(inner_field)
        image_field = remove(apply_shift(first_half) + freq_square * inner_field, orbitals, factor)
        step_size = norm_now / jnp.sum(direction * image_field, axis=(1, 2, 3))
        solution = solution + step_size[:, None, None, None] * direction
        residual = residual - step_size[:, None, None, None] * image_field
        norm_next = jnp.sum(residual * residual, axis=(1, 2, 3))
        direction = residual + (norm_next / norm_now)[:, None, None, None] * direction
        norm_now = norm_next
    response_real = apply_shift(solution)
    density = 4.0 / NOCC * jnp.sum(orbitals * response_real, axis=0)
    return (response_real, density)
```

```python
import functools

import jax
import jax.numpy as jnp
from jax import lax
from jax.experimental import pallas as pl
from jax.experimental.pallas import tpu as pltpu
from jax.sharding import PartitionSpec as P

NOCC = 64
NEAR = 4

kinetic_scale = 0.125
highest = lax.Precision.HIGHEST
f32 = jnp.float32
VMEM = pl.BlockSpec(memory_space=pltpu.VMEM)
SMEM = pl.BlockSpec(memory_space=pltpu.SMEM)


def dot_nn(a, b):
    return lax.dot_general(a, b, (((1,), (0,)), ((), ())), precision=highest, preferred_element_type=f32)


def dot_nt(a, b):
    return lax.dot_general(a, b, (((1,), (1,)), ((), ())), precision=highest, preferred_element_type=f32)


def call(body, args, kinds, outs, scratch=()):
    return pl.pallas_call(
        body,
        in_specs=[SMEM if k == "s" else VMEM for k in kinds],
        out_specs=[VMEM] * len(outs),
        out_shape=[jax.ShapeDtypeStruct(s, f32) for s in outs],
        scratch_shapes=list(scratch),
    )(*args)


def orbital_row_sums(products, own):
    total = functools.reduce(jnp.add, products)
    folded = functools.reduce(jnp.add, [total[i : i + own] for i in range(0, total.shape[0], own)])
    return jnp.sum(folded, axis=1, keepdims=True)


def lane_blocks(ref, cols):
    return [ref[:, i : i + cols] for i in range(0, ref.shape[1], cols)]


def inner_partials(v_ref, stat_refs, w_ref, own, natoms):
    half = stat_refs[0].shape[1]
    sums = sum(
        dot_nt(v_ref[:, h * half : (h + 1) * half], stat_refs[h][0:natoms, :]) for h in range(2)
    )
    planes = w_ref.shape[0]
    return sum(sums[z * own : (z + 1) * own] * w_ref[z : z + 1, :] for z in range(planes))


def pack_edges(v_ref, pc, up_ref, down_ref, own):
    width = v_ref.shape[1]
    up_ref[:, 0:width] = v_ref[v_ref.shape[0] - own :, :]
    up_ref[:, width:] = pc
    down_ref[:, 0:width] = v_ref[0:own, :]
    down_ref[:, width:] = pc


def apply_shift(emit, v_ref, pc_ref, lo_ref, hi_ref, stat_refs, w_ref, coup_ref, en_ref, cols):
    own = lo_ref.shape[0]
    planes = w_ref.shape[0]
    natoms = w_ref.shape[1]
    width = v_ref.shape[1]
    half = width // 2
    c = coup_ref[...] * (pc_ref[...] + lo_ref[:, width:] + hi_ref[:, width:])
    spread = jnp.concatenate([c * w_ref[z : z + 1, :] for z in range(planes)], axis=0)
    shift = jnp.concatenate([6.0 * kinetic_scale - en_ref[...]] * planes, axis=0)
    blocks = width // cols
    for k in range(blocks):
        at = slice(k * cols, (k + 1) * cols)
        stat = stat_refs[k * cols // half]
        inside = (k * cols) % half
        nonlocal_term = dot_nn(spread, stat[0:natoms, inside : inside + cols])
        v = v_ref[:, at]
        after, before = (k + 1) % blocks, (k - 1) % blocks
        beside = v_ref[:, after * cols : (after + 1) * cols] + v_ref[:, before * cols : (before + 1) * cols]
        beside = beside + jnp.concatenate([lo_ref[:, at], v_ref[0 : own * (planes - 1), at]], axis=0)
        beside = beside + jnp.concatenate([v_ref[own:, at], hi_ref[:, at]], axis=0)
        beside = beside + pltpu.roll(v, 1, 1) + pltpu.roll(v, cols - 1, 1)
        local = jnp.concatenate(
            [
                jnp.broadcast_to(stat[natoms + z : natoms + z + 1, inside : inside + cols], (own, cols))
                for z in range(planes)
            ],
            axis=0,
        )
        emit(at, (local + shift) * v - kinetic_scale * beside + nonlocal_term)


def gram_body(where_ref, mine_ref, other_ref, stat_m, stat_o, out_ref, *, own, planes, natoms):
    half = stat_m.shape[1]
    total = mine_ref.shape[0]
    span = total // 2
    rows = pl.ds(pl.multiple_of(where_ref[1] * span, span), span)
    start = pl.multiple_of(where_ref[0], own)
    gram = dot_nt(mine_ref[rows, :], mine_ref[...]) + dot_nt(other_ref[rows, :], other_ref[...])
    corr = jnp.zeros((own, total), f32)
    for orb_ref, stat in ((mine_ref, stat_m), (other_ref, stat_o)):
        for z in range(planes):
            at = slice(z * half, (z + 1) * half)
            source = stat[natoms + planes + z : natoms + planes + z + 1, :] * orb_ref[pl.ds(start, own), at]
            corr = corr + dot_nt(source, orb_ref[:, at])
    quarter = span // 2
    out_ref[0:quarter, :] = jnp.concatenate([gram[0:quarter], gram[quarter:]], axis=1)
    out_ref[quarter:, :] = jnp.concatenate([corr, jnp.zeros((own, total), f32)], axis=1)


def inverse_of(gram):
    n = gram.shape[0]
    eye = (lax.broadcasted_iota(jnp.int32, (n, n), 0) == lax.broadcasted_iota(jnp.int32, (n, n), 1)).astype(f32)
    work = jnp.concatenate([gram, eye], axis=1)
    tiles = [work[i : i + 8] for i in range(0, n, 8)]
    sub = lax.broadcasted_iota(jnp.int32, (8, 2 * n), 0)
    for k in range(n):
        t, r = divmod(k, 8)
        row = tiles[t][r : r + 1, :]
        scaled = row * (1.0 / row[:, k : k + 1])
        scale = lax.rsqrt(row[:, k : k + 1])
        for i in range(t, n // 8):
            step = tiles[i] - tiles[i][:, k : k + 1] * scaled
            if i == t:
                step = jnp.where(sub > r, step, jnp.where(sub == r, tiles[i] * scale, tiles[i]))
            tiles[i] = step
    lower_inverse = jnp.concatenate(tiles, axis=0)[:, n:]
    inv = lax.dot_general(
        lower_inverse, lower_inverse, (((0,), (0,)), ((), ())), precision=highest, preferred_element_type=f32
    )
    return 2.0 * inv - dot_nn(dot_nn(inv, gram), inv)


def source_body(
    where_ref, sums_ref, swapped_ref, mine_ref, other_ref, stat_m, stat_o, w_ref,
    r_ref, up_ref, down_ref, pc_ref, inv_ref, *, own, planes, natoms, cells,
):
    half = stat_m.shape[1]
    total = mine_ref.shape[0]
    quarter = total // 4
    ours, theirs = sums_ref[0:quarter, :], swapped_ref[...]
    first = where_ref[1] == 0
    low, high = jnp.where(first, ours, theirs), jnp.where(first, theirs, ours)
    gram = jnp.concatenate([low[:, :total], low[:, total:], high[:, :total], high[:, total:]], axis=0) / cells
    inv = inverse_of(gram)
    inv_ref[...] = inv
    g = dot_nn(sums_ref[quarter:, 0:total] / cells, inv)
    start = pl.multiple_of(where_ref[0], own)
    for h, (orb_ref, stat) in enumerate(((mine_ref, stat_m), (other_ref, stat_o))):
        for z in range(planes):
            at = slice(z * half, (z + 1) * half)
            source = stat[natoms + planes + z : natoms + planes + z + 1, :] * orb_ref[pl.ds(start, own), at]
            r_ref[z * own : (z + 1) * own, h * half : (h + 1) * half] = dot_nn(g, orb_ref[:, at]) - source
    pc = inner_partials(r_ref, (stat_m, stat_o), w_ref, own, natoms)
    pc_ref[...] = pc
    pack_edges(r_ref, pc, up_ref, down_ref, own)


def first_body(
    v_ref, pc_ref, lo_ref, hi_ref, stat_m, stat_o, w_ref, coup_ref, en_ref,
    f_ref, up_ref, down_ref, out_pc_ref, *, own, natoms, cols,
):
    def emit(at, block):
        f_ref[:, at] = block

    apply_shift(emit, v_ref, pc_ref, lo_ref, hi_ref, (stat_m, stat_o), w_ref, coup_ref, en_ref, cols)
    pc = inner_partials(f_ref, (stat_m, stat_o), w_ref, own, natoms)
    out_pc_ref[...] = pc
    pack_edges(f_ref, pc, up_ref, down_ref, own)


def target_body(
    freq_ref, v_ref, pc_ref, lo_ref, hi_ref, stat_m, stat_o, w_ref, coup_ref, en_ref, r_ref, mine_ref, other_ref,
    t_ref, out_ref, *, own, planes, cols,
):
    square = freq_ref[0] * freq_ref[0]

    def emit(at, block):
        t_ref[:, at] = block + square * r_ref[:, at]

    apply_shift(emit, v_ref, pc_ref, lo_ref, hi_ref, (stat_m, stat_o), w_ref, coup_ref, en_ref, cols)
    half = stat_m.shape[1]
    total = mine_ref.shape[0]
    corr = jnp.zeros((own, total), f32)
    for h, orb_ref in enumerate((mine_ref, other_ref)):
        for z in range(planes):
            block = t_ref[z * own : (z + 1) * own, h * half : (h + 1) * half]
            corr = corr + dot_nt(block, orb_ref[:, z * half : (z + 1) * half])
    rr = orbital_row_sums([b * b for b in lane_blocks(r_ref, cols)], own)
    ff = orbital_row_sums([b * b for b in lane_blocks(v_ref, cols)], own)
    lanes = out_ref.shape[1]
    lane = lax.broadcasted_iota(jnp.int32, (own, lanes), 1)
    spread = jnp.concatenate([corr, jnp.zeros((own, lanes - total), f32)], axis=1)
    out_ref[...] = jnp.where(lane == total, rr, jnp.where(lane == total + 1, ff, spread))


def residual_body(
    freq_ref, sums_ref, inv_ref, r_ref, t_ref, mine_ref, other_ref, stat_m, stat_o, w_ref,
    out_ref, up_ref, down_ref, pc_ref, *, own, planes, natoms, cells,
):
    half = stat_m.shape[1]
    total = mine_ref.shape[0]
    square = freq_ref[0] * freq_ref[0]
    g = dot_nn(sums_ref[:, 0:total] / cells, inv_ref[...])
    rr, ff = sums_ref[:, total : total + 1], sums_ref[:, total + 1 : total + 2]
    step = rr / (ff + square * rr)
    for h, orb_ref in enumerate((mine_ref, other_ref)):
        for z in range(planes):
            rows, at = slice(z * own, (z + 1) * own), slice(h * half, (h + 1) * half)
            image = t_ref[rows, at] - dot_nn(g, orb_ref[:, z * half : (z + 1) * half])
            out_ref[rows, at] = r_ref[rows, at] - step * image
    pc = inner_partials(out_ref, (stat_m, stat_o), w_ref, own, natoms)
    pc_ref[...] = pc
    pack_edges(out_ref, pc, up_ref, down_ref, own)


def last_body(
    v_ref, pc_ref, lo_ref, hi_ref, stat_m, stat_o, w_ref, coup_ref, en_ref, r_ref, f_ref, u_ref, out_ref, *, own, cols
):
    def emit(at, block):
        u_ref[:, at] = block

    apply_shift(emit, v_ref, pc_ref, lo_ref, hi_ref, (stat_m, stat_o), w_ref, coup_ref, en_ref, cols)
    r1, r0, u1, u0 = (lane_blocks(ref, cols) for ref in (v_ref, r_ref, u_ref, f_ref))
    values = [
        orbital_row_sums([a * b for a, b in zip(x, y)], own) for x, y in ((r1, r1), (u1, u1), (u1, u0), (r1, r0))
    ]
    lanes = out_ref.shape[2]
    lane = lax.broadcasted_iota(jnp.int32, (own, lanes), 1)
    row = lax.broadcasted_iota(jnp.int32, (own, lanes), 0)
    placed = sum(jnp.where(lane == own * s + row, value, 0.0) for s, value in enumerate(values))
    line = jnp.sum(placed, axis=0, keepdims=True)
    out_ref[...] = jnp.broadcast_to(line[None], out_ref.shape)


def response_body(
    where_ref, freq_ref, sums_ref, lines_ref, f_ref, u_ref, mine_ref, other_ref, out_ref, swap_ref, dens_ref, *, own, planes
):
    total = mine_ref.shape[0]
    half = f_ref.shape[1] // 2
    square = freq_ref[0] * freq_ref[0]
    rr0, ff = sums_ref[:, total : total + 1], sums_ref[:, total + 1 : total + 2]
    line = jnp.sum(lines_ref[...], axis=0)[0:1, :]
    lanes = line.shape[1]
    lane = lax.broadcasted_iota(jnp.int32, (own, lanes), 1)
    row = lax.broadcasted_iota(jnp.int32, (own, lanes), 0)
    rr1, uu, uf, rx = (
        jnp.sum(jnp.where(lane == own * s + row, line, 0.0), axis=1, keepdims=True) for s in range(4)
    )
    step0 = rr0 / (ff + square * rr0)
    beta = rr1 / rr0
    curvature = uu + 2.0 * beta * uf + beta * beta * ff + square * (rr1 + 2.0 * beta * rx + beta * beta * rr0)
    step1 = rr1 / curvature
    start = pl.multiple_of(where_ref[0], own)
    swap_ref[own:, :] = jnp.zeros((swap_ref.shape[0] - own, swap_ref.shape[1]), f32)
    for h, orb_ref in enumerate((mine_ref, other_ref)):
        for z in range(planes):
            rows, at = slice(z * own, (z + 1) * own), slice(h * half, (h + 1) * half)
            to = slice(z * half, (z + 1) * half)
            response = (step0 + step1 * beta) * f_ref[rows, at] + step1 * u_ref[rows, at]
            dens = jnp.sum(orb_ref[pl.ds(start, own), to] * response, axis=0, keepdims=True)
            if h == 0:
                out_ref[:, to] = response
                dens_ref[:, to] = dens
            else:
                swap_ref[0:own, to] = response
                swap_ref[own : own + 1, to] = dens


def copy_for_each(array, axis):
    copies = jnp.broadcast_to(array, (lax.axis_size(axis), *array.shape))
    return lax.all_to_all(copies, axis, split_axis=0, concat_axis=0, tiled=True)


def swap_cores(array):
    return lax.ppermute(array, "pen", [(0, 1), (1, 0)])


def summed(array):
    count = lax.axis_size("slab")
    runs = [[i + j for j in range(NEAR)] for i in range(0, count, NEAR)]
    across = [[i + j for i in range(0, count, NEAR)] for j in range(NEAR)]
    array = lax.psum(array, "slab", axis_index_groups=runs)
    return lax.psum(array, "slab", axis_index_groups=across)


def from_neighbours(up, down):
    count = lax.axis_size("slab")
    ring = [(i, (i + 1) % count) for i in range(count)]
    return lax.ppermute(up, "slab", ring), lax.ppermute(down, "slab", [(b, a) for a, b in ring])


def plane_weights(atom_planes, profiles, planes, depth_total):
    span_size = profiles.shape[1]
    covered = (atom_planes[:, None] + jnp.arange(span_size, dtype=jnp.int32)[None, :]) % depth_total
    matches = (covered[None, :, :] == planes[:, None, None]).astype(jnp.float32)
    return jnp.sum(profiles[None, :, :] * matches, axis=2)


def on_device(
    orbitals, energies, frequency, local_potential, perturbation, projectors, profiles, couplings, atom_planes
):
    chip_count, planes, row_count, cols = orbitals.shape
    natoms = projectors.shape[0]
    half = row_count * cols
    slabs = lax.axis_size("slab")
    assert lax.axis_size("pen") == 2 and slabs > 2
    assert profiles.shape[1] == planes + 1
    depth_total = planes * slabs
    cells = float(depth_total * 2 * half)
    own = chip_count // 2
    core = lax.axis_index("pen")
    first_plane = lax.axis_index("slab") * planes
    weights = plane_weights(atom_planes, profiles, first_plane + jnp.arange(planes, dtype=jnp.int32), depth_total)
    where = jnp.stack([lax.axis_index("orb") * chip_count + core * own, core]).astype(jnp.int32)
    own_energies = lax.dynamic_slice(energies, (core * own,), (own,)).reshape(own, 1)
    coup = couplings.reshape(1, natoms)

    stat_m = jnp.concatenate(
        [a.reshape(-1, half) for a in (projectors, local_potential, perturbation)], axis=0
    )
    stat_o = swap_cores(stat_m)
    mine = copy_for_each(orbitals.reshape(chip_count, planes * half), "orb").reshape(-1, planes * half)
    other = swap_cores(mine)
    total = mine.shape[0]
    stats = (stat_m, stat_o)
    field, edge, part = (planes * own, 2 * half), (own, 2 * half + natoms), (own, natoms)

    (gram_part,) = call(
        functools.partial(gram_body, own=own, planes=planes, natoms=natoms),
        (where, mine, other, *stats), "svvvv", [(total // 4 + own, 2 * total)],
    )
    gram_sum = summed(gram_part)
    gram_other = swap_cores(gram_sum[0 : total // 4])
    r0, up, down, pc, inv = call(
        functools.partial(source_body, own=own, planes=planes, natoms=natoms, cells=cells),
        (where, gram_sum, gram_other, mine, other, *stats, weights), "svvvvvvv",
        [field, edge, edge, part, (total, total)],
    )
    lo, hi = from_neighbours(up, down)
    first, up, down, first_pc = call(
        functools.partial(first_body, own=own, natoms=natoms, cols=cols),
        (r0, pc, lo, hi, *stats, weights, coup, own_energies), "v" * 9, [field, edge, edge, part],
    )
    lo, hi = from_neighbours(up, down)
    target, sums_part = call(
        functools.partial(target_body, own=own, planes=planes, cols=cols),
        (frequency, first, first_pc, lo, hi, *stats, weights, coup, own_energies, r0, mine, other), "s" + "v" * 12,
        [field, (own, 2 * total)],
    )
    sums = summed(sums_part)
    r1, up, down, pc = call(
        functools.partial(residual_body, own=own, planes=planes, natoms=natoms, cells=cells),
        (frequency, sums, inv, r0, target, mine, other, *stats, weights), "s" + "v" * 9, [field, edge, edge, part],
    )
    lo, hi = from_neighbours(up, down)
    last, lines = call(
        functools.partial(last_body, own=own, cols=cols),
        (r1, pc, lo, hi, *stats, weights, coup, own_energies, r0, first), "v" * 11,
        [field, (slabs, 2, 2 * total)],
    )
    lines = lax.all_to_all(lines, "slab", split_axis=0, concat_axis=0, tiled=True)
    response, to_other, dens = call(
        functools.partial(response_body, own=own, planes=planes),
        (where, frequency, sums, lines, first, last, mine, other), "ss" + "v" * 6,
        [(own, planes * half), (2 * own, planes * half), (1, planes * half)],
    )
    got = swap_cores(to_other)
    theirs = got[0:own]
    low, high = jnp.where(core == 0, response, theirs), jnp.where(core == 0, theirs, response)
    response_real = jnp.concatenate([low, high], axis=0).reshape(orbitals.shape)
    dens = (dens + got[own : own + 1]).reshape(planes, half)
    density = copy_for_each(dens, "orb").sum(axis=0) * (4.0 / NOCC)
    return response_real, density.reshape(planes, row_count, cols)


def solution(mesh):
    in_specs = (
        P(("parts", "orb"), "slab", "pen", None),
        P(("parts", "orb")),
        P("parts"),
        P("slab", "pen", None),
        P("slab", "pen", None),
        P(None, "pen", None),
        P(),
        P(),
        P(),
    )
    out_specs = (P(("parts", "orb"), "slab", "pen", None), P(("parts", "slab"), "pen", None))
    return jax.shard_map(on_device, mesh=mesh, in_specs=in_specs, out_specs=out_specs, check_vma=False)
```

```python
import functools

import jax
import jax.numpy as jnp
from jax import lax
from jax.experimental import pallas as pl
from jax.experimental.pallas import tpu as pltpu
from jax.sharding import PartitionSpec as P

NOCC = 64
NEAR = 4

kinetic_scale = 0.125
highest = lax.Precision.HIGHEST
f32 = jnp.float32
VMEM = pl.BlockSpec(memory_space=pltpu.VMEM)
SMEM = pl.BlockSpec(memory_space=pltpu.SMEM)


def dot_nn(a, b):
    return lax.dot_general(a, b, (((1,), (0,)), ((), ())), precision=highest, preferred_element_type=f32)


def dot_nt(a, b):
    return lax.dot_general(a, b, (((1,), (1,)), ((), ())), precision=highest, preferred_element_type=f32)


def call(body, args, kinds, outs):
    args = [pltpu.with_memory_space_constraint(a, pltpu.VMEM) if k == "k" else a for a, k in zip(args, kinds, strict=True)]
    return pl.pallas_call(
        body,
        in_specs=[SMEM if k == "s" else VMEM for k in kinds],
        out_specs=[VMEM] * len(outs),
        out_shape=[pltpu.VMEM(s, f32) for s in outs],
    )(*args)


def orbital_row_sums(products, own):
    total = functools.reduce(jnp.add, products)
    folded = functools.reduce(jnp.add, [total[i : i + own] for i in range(0, total.shape[0], own)])
    return jnp.sum(folded, axis=1, keepdims=True)


def lane_blocks(ref, cols):
    return [ref[:, i : i + cols] for i in range(0, ref.shape[1], cols)]


def inner_partials(v_ref, stat_refs, w_ref, own, natoms):
    half = stat_refs[0].shape[1]
    sums = sum(
        dot_nt(v_ref[:, h * half : (h + 1) * half], stat_refs[h][0:natoms, :]) for h in range(2)
    )
    planes = w_ref.shape[0]
    return sum(sums[z * own : (z + 1) * own] * w_ref[z : z + 1, :] for z in range(planes))


def pack_edges(v_ref, pc, up_ref, down_ref, own):
    width = v_ref.shape[1]
    up_ref[:, 0:width] = v_ref[v_ref.shape[0] - own :, :]
    up_ref[:, width:] = pc
    down_ref[:, 0:width] = v_ref[0:own, :]
    down_ref[:, width:] = pc


def apply_shift(emit, v_ref, pc_ref, lo_ref, hi_ref, stat_refs, w_ref, coup_ref, en_ref, cols):
    own = lo_ref.shape[0]
    planes = w_ref.shape[0]
    natoms = w_ref.shape[1]
    width = v_ref.shape[1]
    half = width // 2
    c = coup_ref[...] * (pc_ref[...] + lo_ref[:, width:] + hi_ref[:, width:])
    spread = jnp.concatenate([c * w_ref[z : z + 1, :] for z in range(planes)], axis=0)
    shift = jnp.concatenate([6.0 * kinetic_scale - en_ref[...]] * planes, axis=0)
    blocks = width // cols
    for k in range(blocks):
        at = slice(k * cols, (k + 1) * cols)
        stat = stat_refs[k * cols // half]
        inside = (k * cols) % half
        nonlocal_term = dot_nn(spread, stat[0:natoms, inside : inside + cols])
        v = v_ref[:, at]
        after, before = (k + 1) % blocks, (k - 1) % blocks
        beside = v_ref[:, after * cols : (after + 1) * cols] + v_ref[:, before * cols : (before + 1) * cols]
        beside = beside + jnp.concatenate([lo_ref[:, at], v_ref[0 : own * (planes - 1), at]], axis=0)
        beside = beside + jnp.concatenate([v_ref[own:, at], hi_ref[:, at]], axis=0)
        beside = beside + pltpu.roll(v, 1, 1) + pltpu.roll(v, cols - 1, 1)
        local = jnp.concatenate(
            [
                jnp.broadcast_to(stat[natoms + z : natoms + z + 1, inside : inside + cols], (own, cols))
                for z in range(planes)
            ],
            axis=0,
        )
        emit(at, (local + shift) * v - kinetic_scale * beside + nonlocal_term)


def gram_body(where_ref, mine_ref, other_ref, stat_m, stat_o, out_ref, *, own, planes, natoms):
    half = stat_m.shape[1]
    total = mine_ref.shape[0]
    span, quarter = total // 2, total // 4
    rows = pl.ds(pl.multiple_of(where_ref[1] * span, span), span)
    start = pl.multiple_of(where_ref[0], own)
    sums = jnp.zeros((span + own, total), f32)
    for orb_ref, stat in ((mine_ref, stat_m), (other_ref, stat_o)):
        for z in range(planes):
            at = slice(z * half, (z + 1) * half)
            source = stat[natoms + planes + z : natoms + planes + z + 1, :] * orb_ref[pl.ds(start, own), at]
            sums = sums + dot_nt(jnp.concatenate([orb_ref[rows, at], source], axis=0), orb_ref[:, at])
    gram, corr = sums[0:span], sums[span:]
    twice = jnp.concatenate([gram, gram], axis=1)
    ahead = jnp.where(where_ref[1] == 0, twice[:, 0:total], twice[:, span : span + total])
    out_ref[...] = jnp.concatenate(
        [
            ahead[0:quarter, 0 : 3 * quarter],
            ahead[quarter:, quarter:],
            jnp.concatenate([corr[:, 0:span], corr[:, span:]], axis=0),
        ],
        axis=1,
    )


def gram_from(low, high):
    quarter = low.shape[0]
    blocks = [
        [part[:, i + d * quarter : i + (d + 1) * quarter] * (1.0 if d == 1 else 0.5) for d in range(3)]
        + [jnp.zeros((quarter, quarter), f32)]
        for part in (low, high)
        for i in (0, 3 * quarter)
    ]
    upper = jnp.concatenate(
        [jnp.concatenate([blocks[j][(k - j) % 4] for k in range(4)], axis=1) for j in range(4)], axis=0
    )
    return upper + upper.T


def inverse_of(gram):
    n = gram.shape[0]
    eye = (lax.broadcasted_iota(jnp.int32, (n, n), 0) == lax.broadcasted_iota(jnp.int32, (n, n), 1)).astype(f32)
    work = jnp.concatenate([gram, eye], axis=1)
    tiles = [work[i : i + 8] for i in range(0, n, 8)]
    sub = lax.broadcasted_iota(jnp.int32, (8, 2 * n), 0)
    for k in range(0, n, 2):
        t, r = divmod(k, 8)
        row0, row1 = tiles[t][r : r + 1, :], tiles[t][r + 1 : r + 2, :]
        a, b, d = row0[:, k : k + 1], row0[:, k + 1 : k + 2], row1[:, k + 1 : k + 2]
        det = a * d - b * b
        over = 1.0 / det
        x0 = row0 * (d * over) - row1 * (b * over)
        x1 = row1 * (a * over) - row0 * (b * over)
        for i in range(t, n // 8):
            step = tiles[i] - tiles[i][:, k : k + 1] * x0 - tiles[i][:, k + 1 : k + 2] * x1
            if i == t:
                first = row0 * lax.rsqrt(a)
                second = (row1 - row0 * (b / a)) * lax.rsqrt(det / a)
                kept = jnp.where(sub == r, first, jnp.where(sub == r + 1, second, tiles[i]))
                step = jnp.where(sub > r + 1, step, kept)
            tiles[i] = step
    lower_inverse = jnp.concatenate(tiles, axis=0)[:, n:]
    inv = lax.dot_general(
        lower_inverse, lower_inverse, (((0,), (0,)), ((), ())), precision=highest, preferred_element_type=f32
    )
    return 2.0 * inv - dot_nn(dot_nn(inv, gram), inv)


def source_body(
    where_ref, sums_ref, swapped_ref, mine_ref, other_ref, stat_m, stat_o, w_ref,
    r_ref, up_ref, down_ref, pc_ref, inv_ref, *, own, planes, natoms, cells,
):
    half = stat_m.shape[1]
    total = mine_ref.shape[0]
    ours, theirs = sums_ref[...], swapped_ref[...]
    first = where_ref[1] == 0
    gram = gram_from(jnp.where(first, ours, theirs), jnp.where(first, theirs, ours)) / cells
    inv = inverse_of(gram)
    inv_ref[...] = inv
    folded = ours[:, 2 * total - total // 2 :] / cells
    g = dot_nn(jnp.concatenate([folded[0:own], folded[own:]], axis=1), inv)
    start = pl.multiple_of(where_ref[0], own)
    for h, (orb_ref, stat) in enumerate(((mine_ref, stat_m), (other_ref, stat_o))):
        for z in range(planes):
            at = slice(z * half, (z + 1) * half)
            source = stat[natoms + planes + z : natoms + planes + z + 1, :] * orb_ref[pl.ds(start, own), at]
            r_ref[z * own : (z + 1) * own, h * half : (h + 1) * half] = dot_nn(g, orb_ref[:, at]) - source
    pc = inner_partials(r_ref, (stat_m, stat_o), w_ref, own, natoms)
    pc_ref[...] = pc
    pack_edges(r_ref, pc, up_ref, down_ref, own)


def first_body(
    v_ref, pc_ref, lo_ref, hi_ref, stat_m, stat_o, w_ref, coup_ref, en_ref,
    f_ref, up_ref, down_ref, out_pc_ref, *, own, natoms, cols,
):
    def emit(at, block):
        f_ref[:, at] = block

    apply_shift(emit, v_ref, pc_ref, lo_ref, hi_ref, (stat_m, stat_o), w_ref, coup_ref, en_ref, cols)
    pc = inner_partials(f_ref, (stat_m, stat_o), w_ref, own, natoms)
    out_pc_ref[...] = pc
    pack_edges(f_ref, pc, up_ref, down_ref, own)


def target_body(
    freq_ref, v_ref, pc_ref, lo_ref, hi_ref, stat_m, stat_o, w_ref, coup_ref, en_ref, r_ref, mine_ref, other_ref,
    t_ref, out_ref, *, own, planes, cols,
):
    square = freq_ref[0] * freq_ref[0]

    def emit(at, block):
        t_ref[:, at] = block + square * r_ref[:, at]

    apply_shift(emit, v_ref, pc_ref, lo_ref, hi_ref, (stat_m, stat_o), w_ref, coup_ref, en_ref, cols)
    half = stat_m.shape[1]
    total = mine_ref.shape[0]
    corr = jnp.zeros((own, total), f32)
    for h, orb_ref in enumerate((mine_ref, other_ref)):
        for z in range(planes):
            block = t_ref[z * own : (z + 1) * own, h * half : (h + 1) * half]
            corr = corr + dot_nt(block, orb_ref[:, z * half : (z + 1) * half])
    rr = orbital_row_sums([b * b for b in lane_blocks(r_ref, cols)], own)
    ff = orbital_row_sums([b * b for b in lane_blocks(v_ref, cols)], own)
    lanes = out_ref.shape[1]
    lane = lax.broadcasted_iota(jnp.int32, (own, lanes), 1)
    spread = jnp.concatenate([corr, jnp.zeros((own, lanes - total), f32)], axis=1)
    out_ref[...] = jnp.where(lane == total, rr, jnp.where(lane == total + 1, ff, spread))


def residual_body(
    freq_ref, sums_ref, inv_ref, r_ref, t_ref, mine_ref, other_ref, stat_m, stat_o, w_ref,
    out_ref, up_ref, down_ref, pc_ref, *, own, planes, natoms, cells,
):
    half = stat_m.shape[1]
    total = mine_ref.shape[0]
    square = freq_ref[0] * freq_ref[0]
    g = dot_nn(sums_ref[:, 0:total] / cells, inv_ref[...])
    rr, ff = sums_ref[:, total : total + 1], sums_ref[:, total + 1 : total + 2]
    step = rr / (ff + square * rr)
    for h, orb_ref in enumerate((mine_ref, other_ref)):
        for z in range(planes):
            rows, at = slice(z * own, (z + 1) * own), slice(h * half, (h + 1) * half)
            image = t_ref[rows, at] - dot_nn(g, orb_ref[:, z * half : (z + 1) * half])
            out_ref[rows, at] = r_ref[rows, at] - step * image
    pc = inner_partials(out_ref, (stat_m, stat_o), w_ref, own, natoms)
    pc_ref[...] = pc
    pack_edges(out_ref, pc, up_ref, down_ref, own)


def last_body(
    v_ref, pc_ref, lo_ref, hi_ref, stat_m, stat_o, w_ref, coup_ref, en_ref, r_ref, f_ref, u_ref, out_ref, *, own, cols
):
    def emit(at, block):
        u_ref[:, at] = block

    apply_shift(emit, v_ref, pc_ref, lo_ref, hi_ref, (stat_m, stat_o), w_ref, coup_ref, en_ref, cols)
    r1, r0, u1, u0 = (lane_blocks(ref, cols) for ref in (v_ref, r_ref, u_ref, f_ref))
    values = [
        orbital_row_sums([a * b for a, b in zip(x, y)], own) for x, y in ((r1, r1), (u1, u1), (u1, u0), (r1, r0))
    ]
    lanes = out_ref.shape[2]
    lane = lax.broadcasted_iota(jnp.int32, (own, lanes), 1)
    row = lax.broadcasted_iota(jnp.int32, (own, lanes), 0)
    placed = sum(jnp.where(lane == own * s + row, value, 0.0) for s, value in enumerate(values))
    line = jnp.sum(placed, axis=0, keepdims=True)
    out_ref[...] = jnp.broadcast_to(line[None], out_ref.shape)


def response_body(
    where_ref, freq_ref, sums_ref, lines_ref, f_ref, u_ref, mine_ref, other_ref, out_ref, swap_ref, dens_ref, *, own, planes
):
    total = mine_ref.shape[0]
    half = f_ref.shape[1] // 2
    square = freq_ref[0] * freq_ref[0]
    rr0, ff = sums_ref[:, total : total + 1], sums_ref[:, total + 1 : total + 2]
    line = jnp.sum(lines_ref[...], axis=0)[0:1, :]
    lanes = line.shape[1]
    lane = lax.broadcasted_iota(jnp.int32, (own, lanes), 1)
    row = lax.broadcasted_iota(jnp.int32, (own, lanes), 0)
    rr1, uu, uf, rx = (
        jnp.sum(jnp.where(lane == own * s + row, line, 0.0), axis=1, keepdims=True) for s in range(4)
    )
    step0 = rr0 / (ff + square * rr0)
    beta = rr1 / rr0
    curvature = uu + 2.0 * beta * uf + beta * beta * ff + square * (rr1 + 2.0 * beta * rx + beta * beta * rr0)
    step1 = rr1 / curvature
    start = pl.multiple_of(where_ref[0], own)
    swap_ref[own:, :] = jnp.zeros((swap_ref.shape[0] - own, swap_ref.shape[1]), f32)
    for h, orb_ref in enumerate((mine_ref, other_ref)):
        for z in range(planes):
            rows, at = slice(z * own, (z + 1) * own), slice(h * half, (h + 1) * half)
            to = slice(z * half, (z + 1) * half)
            response = (step0 + step1 * beta) * f_ref[rows, at] + step1 * u_ref[rows, at]
            dens = jnp.sum(orb_ref[pl.ds(start, own), to] * response, axis=0, keepdims=True)
            if h == 0:
                out_ref[:, to] = response
                dens_ref[:, to] = dens
            else:
                swap_ref[0:own, to] = response
                swap_ref[own : own + 1, to] = dens


def copy_for_each(array, axis):
    copies = jnp.broadcast_to(array, (lax.axis_size(axis), *array.shape))
    return lax.all_to_all(copies, axis, split_axis=0, concat_axis=0, tiled=True)


def swap_cores(array):
    return lax.ppermute(array, "pen", [(0, 1), (1, 0)])


def summed(array):
    count = lax.axis_size("slab")
    runs = [[i + j for j in range(NEAR)] for i in range(0, count, NEAR)]
    across = [[i + j for i in range(0, count, NEAR)] for j in range(NEAR)]
    array = lax.psum(array, "slab", axis_index_groups=runs)
    return lax.psum(array, "slab", axis_index_groups=across)


def from_neighbours(up, down):
    count = lax.axis_size("slab")
    ring = [(i, (i + 1) % count) for i in range(count)]
    return lax.ppermute(up, "slab", ring), lax.ppermute(down, "slab", [(b, a) for a, b in ring])


def plane_weights(atom_planes, profiles, planes, depth_total):
    span_size = profiles.shape[1]
    covered = (atom_planes[:, None] + jnp.arange(span_size, dtype=jnp.int32)[None, :]) % depth_total
    matches = (covered[None, :, :] == planes[:, None, None]).astype(jnp.float32)
    return jnp.sum(profiles[None, :, :] * matches, axis=2)


def on_device(
    orbitals, energies, frequency, local_potential, perturbation, projectors, profiles, couplings, atom_planes
):
    chip_count, planes, row_count, cols = orbitals.shape
    natoms = projectors.shape[0]
    half = row_count * cols
    slabs = lax.axis_size("slab")
    assert lax.axis_size("pen") == 2 and slabs > 2
    assert profiles.shape[1] == planes + 1
    depth_total = planes * slabs
    cells = float(depth_total * 2 * half)
    own = chip_count // 2
    core = lax.axis_index("pen")
    first_plane = lax.axis_index("slab") * planes
    weights = plane_weights(atom_planes, profiles, first_plane + jnp.arange(planes, dtype=jnp.int32), depth_total)
    where = jnp.stack([lax.axis_index("orb") * chip_count + core * own, core]).astype(jnp.int32)
    own_energies = lax.dynamic_slice(energies, (core * own,), (own,)).reshape(own, 1)
    coup = couplings.reshape(1, natoms)

    stat_m = jnp.concatenate(
        [a.reshape(-1, half) for a in (projectors, local_potential, perturbation)], axis=0
    )
    stat_o = swap_cores(stat_m)
    mine = copy_for_each(orbitals.reshape(chip_count, planes * half), "orb").reshape(-1, planes * half)
    other = swap_cores(mine)
    total = mine.shape[0]
    stats = (stat_m, stat_o)
    field, edge, part = (planes * own, 2 * half), (own, 2 * half + natoms), (own, natoms)

    (gram_part,) = call(
        functools.partial(gram_body, own=own, planes=planes, natoms=natoms),
        (where, mine, other, *stats), "svvkk", [(total // 4, 2 * total)],
    )
    gram_sum = summed(gram_part)
    gram_other = swap_cores(gram_sum)
    r0, up, down, pc, inv = call(
        functools.partial(source_body, own=own, planes=planes, natoms=natoms, cells=cells),
        (where, gram_sum, gram_other, mine, other, *stats, weights), "skkvvkkk",
        [field, edge, edge, part, (total, total)],
    )
    lo, hi = from_neighbours(up, down)
    first, up, down, first_pc = call(
        functools.partial(first_body, own=own, natoms=natoms, cols=cols),
        (r0, pc, lo, hi, *stats, weights, coup, own_energies), "kkkkkkkkk", [field, edge, edge, part],
    )
    lo, hi = from_neighbours(up, down)
    target, sums_part = call(
        functools.partial(target_body, own=own, planes=planes, cols=cols),
        (frequency, first, first_pc, lo, hi, *stats, weights, coup, own_energies, r0, mine, other), "skkkkkkkkkkvv",
        [field, (own, 2 * total)],
    )
    sums = summed(sums_part)
    r1, up, down, pc = call(
        functools.partial(residual_body, own=own, planes=planes, natoms=natoms, cells=cells),
        (frequency, sums, inv, r0, target, mine, other, *stats, weights), "skkkkvvkkk", [field, edge, edge, part],
    )
    lo, hi = from_neighbours(up, down)
    last, lines = call(
        functools.partial(last_body, own=own, cols=cols),
        (r1, pc, lo, hi, *stats, weights, coup, own_energies, r0, first), "kkkkkkkkkkk",
        [field, (slabs, 2, 2 * total)],
    )
    lines = lax.all_to_all(lines, "slab", split_axis=0, concat_axis=0, tiled=True)
    response, to_other, dens = call(
        functools.partial(response_body, own=own, planes=planes),
        (where, frequency, sums, lines, first, last, mine, other), "sskkkkvv",
        [(own, planes * half), (2 * own, planes * half), (1, planes * half)],
    )
    got = swap_cores(to_other)
    theirs = got[0:own]
    low, high = jnp.where(core == 0, response, theirs), jnp.where(core == 0, theirs, response)
    response_real = jnp.concatenate([low, high], axis=0).reshape(orbitals.shape)
    dens = (dens + got[own : own + 1]).reshape(planes, half)
    density = copy_for_each(dens, "orb").sum(axis=0) * (4.0 / NOCC)
    return response_real, density.reshape(planes, row_count, cols)


def solution(mesh):
    in_specs = (
        P(("parts", "orb"), "slab", "pen", None),
        P(("parts", "orb")),
        P("parts"),
        P("slab", "pen", None),
        P("slab", "pen", None),
        P(None, "pen", None),
        P(),
        P(),
        P(),
    )
    out_specs = (P(("parts", "orb"), "slab", "pen", None), P(("parts", "slab"), "pen", None))
    return jax.shard_map(on_device, mesh=mesh, in_specs=in_specs, out_specs=out_specs, check_vma=False)
```

```python
import functools

import jax
import jax.numpy as jnp
from jax import lax
from jax.experimental import pallas as pl
from jax.experimental.pallas import tpu as pltpu
from jax.sharding import PartitionSpec as P

NOCC = 64
NEAR = 4

kinetic_scale = 0.125
highest = lax.Precision.HIGHEST
f32 = jnp.float32
VMEM = pl.BlockSpec(memory_space=pltpu.VMEM)
SMEM = pl.BlockSpec(memory_space=pltpu.SMEM)


def dot_nn(a, b):
    return lax.dot_general(a, b, (((1,), (0,)), ((), ())), precision=highest, preferred_element_type=f32)


def dot_nt(a, b):
    return lax.dot_general(a, b, (((1,), (1,)), ((), ())), precision=highest, preferred_element_type=f32)


def call(body, args, kinds, outs):
    args = [pltpu.with_memory_space_constraint(a, pltpu.VMEM) if k == "k" else a for a, k in zip(args, kinds, strict=True)]
    return pl.pallas_call(
        body,
        in_specs=[SMEM if k == "s" else VMEM for k in kinds],
        out_specs=[VMEM] * len(outs),
        out_shape=[pltpu.VMEM(s, f32) for s in outs],
    )(*args)


def orbital_row_sums(products, own):
    total = functools.reduce(jnp.add, products)
    folded = functools.reduce(jnp.add, [total[i : i + own] for i in range(0, total.shape[0], own)])
    return jnp.sum(folded, axis=1, keepdims=True)


def lane_blocks(ref, cols):
    return [ref[:, i : i + cols] for i in range(0, ref.shape[1], cols)]


def inner_partials(v_ref, stat_refs, w_ref, own, natoms):
    half = stat_refs[0].shape[1]
    sums = sum(
        dot_nt(v_ref[:, h * half : (h + 1) * half], stat_refs[h][0:natoms, :]) for h in range(2)
    )
    planes = w_ref.shape[0]
    return sum(sums[z * own : (z + 1) * own] * w_ref[z : z + 1, :] for z in range(planes))


def pack_edges(where_ref, v_ref, pc, up_ref, down_ref, own):
    width = v_ref.shape[1]
    half = width // 2
    for ref, edge, crossing in (
        (up_ref, v_ref[v_ref.shape[0] - own :, :], where_ref[2] == 1),
        (down_ref, v_ref[0:own, :], where_ref[3] == 1),
    ):
        ref[:, 0:half] = jnp.where(crossing, edge[:, half:], edge[:, 0:half])
        ref[:, half:width] = jnp.where(crossing, edge[:, 0:half], edge[:, half:])
        ref[:, width:] = pc


def apply_shift(emit, v_ref, pc_ref, lo_ref, hi_ref, stat_refs, w_ref, coup_ref, en_ref, cols):
    own = lo_ref.shape[0]
    planes = w_ref.shape[0]
    natoms = w_ref.shape[1]
    width = v_ref.shape[1]
    half = width // 2
    c = coup_ref[...] * (pc_ref[...] + lo_ref[:, width:] + hi_ref[:, width:])
    spread = jnp.concatenate([c * w_ref[z : z + 1, :] for z in range(planes)], axis=0)
    shift = jnp.concatenate([6.0 * kinetic_scale - en_ref[...]] * planes, axis=0)
    blocks = width // cols
    for k in range(blocks):
        at = slice(k * cols, (k + 1) * cols)
        stat = stat_refs[k * cols // half]
        inside = (k * cols) % half
        nonlocal_term = dot_nn(spread, stat[0:natoms, inside : inside + cols])
        v = v_ref[:, at]
        after, before = (k + 1) % blocks, (k - 1) % blocks
        beside = v_ref[:, after * cols : (after + 1) * cols] + v_ref[:, before * cols : (before + 1) * cols]
        beside = beside + jnp.concatenate([lo_ref[:, at], v_ref[0 : own * (planes - 1), at]], axis=0)
        beside = beside + jnp.concatenate([v_ref[own:, at], hi_ref[:, at]], axis=0)
        beside = beside + pltpu.roll(v, 1, 1) + pltpu.roll(v, cols - 1, 1)
        local = jnp.concatenate(
            [
                jnp.broadcast_to(stat[natoms + z : natoms + z + 1, inside : inside + cols], (own, cols))
                for z in range(planes)
            ],
            axis=0,
        )
        emit(at, (local + shift) * v - kinetic_scale * beside + nonlocal_term)


def gram_body(where_ref, mine_ref, other_ref, stat_m, stat_o, out_ref, *, own, planes, natoms):
    half = stat_m.shape[1]
    total = mine_ref.shape[0]
    span, quarter = total // 2, total // 4
    rows = pl.ds(pl.multiple_of(where_ref[1] * span, span), span)
    start = pl.multiple_of(where_ref[0], own)
    sums = jnp.zeros((span + own, total), f32)
    for orb_ref, stat in ((mine_ref, stat_m), (other_ref, stat_o)):
        for z in range(planes):
            at = slice(z * half, (z + 1) * half)
            source = stat[natoms + planes + z : natoms + planes + z + 1, :] * orb_ref[pl.ds(start, own), at]
            sums = sums + dot_nt(jnp.concatenate([orb_ref[rows, at], source], axis=0), orb_ref[:, at])
    gram, corr = sums[0:span], sums[span:]
    twice = jnp.concatenate([gram, gram], axis=1)
    ahead = jnp.where(where_ref[1] == 0, twice[:, 0:total], twice[:, span : span + total])
    out_ref[...] = jnp.concatenate(
        [
            ahead[0:quarter, 0 : 3 * quarter],
            ahead[quarter:, quarter:],
            jnp.concatenate([corr[:, 0:span], corr[:, span:]], axis=0),
        ],
        axis=1,
    )


def gram_from(low, high):
    quarter = low.shape[0]
    blocks = [
        [part[:, i + d * quarter : i + (d + 1) * quarter] * (1.0 if d == 1 else 0.5) for d in range(3)]
        + [jnp.zeros((quarter, quarter), f32)]
        for part in (low, high)
        for i in (0, 3 * quarter)
    ]
    upper = jnp.concatenate(
        [jnp.concatenate([blocks[j][(k - j) % 4] for k in range(4)], axis=1) for j in range(4)], axis=0
    )
    return upper + upper.T


def inverse_of(gram):
    n = gram.shape[0]
    eye = (lax.broadcasted_iota(jnp.int32, (n, n), 0) == lax.broadcasted_iota(jnp.int32, (n, n), 1)).astype(f32)
    work = jnp.concatenate([gram, eye], axis=1)
    tiles = [work[i : i + 8] for i in range(0, n, 8)]
    sub = lax.broadcasted_iota(jnp.int32, (8, 2 * n), 0)
    for k in range(0, n, 2):
        t, r = divmod(k, 8)
        row0, row1 = tiles[t][r : r + 1, :], tiles[t][r + 1 : r + 2, :]
        a, b, d = row0[:, k : k + 1], row0[:, k + 1 : k + 2], row1[:, k + 1 : k + 2]
        det = a * d - b * b
        over = 1.0 / det
        x0 = row0 * (d * over) - row1 * (b * over)
        x1 = row1 * (a * over) - row0 * (b * over)
        for i in range(t, n // 8):
            step = tiles[i] - tiles[i][:, k : k + 1] * x0 - tiles[i][:, k + 1 : k + 2] * x1
            if i == t:
                first = row0 * lax.rsqrt(a)
                second = (row1 - row0 * (b / a)) * lax.rsqrt(det / a)
                kept = jnp.where(sub == r, first, jnp.where(sub == r + 1, second, tiles[i]))
                step = jnp.where(sub > r + 1, step, kept)
            tiles[i] = step
    lower_inverse = jnp.concatenate(tiles, axis=0)[:, n:]
    inv = lax.dot_general(
        lower_inverse, lower_inverse, (((0,), (0,)), ((), ())), precision=highest, preferred_element_type=f32
    )
    return 2.0 * inv - dot_nn(dot_nn(inv, gram), inv)


def source_body(
    where_ref, sums_ref, swapped_ref, mine_ref, other_ref, stat_m, stat_o, w_ref,
    r_ref, up_ref, down_ref, pc_ref, inv_ref, *, own, planes, natoms, cells,
):
    half = stat_m.shape[1]
    total = mine_ref.shape[0]
    ours, theirs = sums_ref[...], swapped_ref[...]
    first = where_ref[1] == 0
    gram = gram_from(jnp.where(first, ours, theirs), jnp.where(first, theirs, ours)) / cells
    inv = inverse_of(gram)
    inv_ref[...] = inv
    folded = ours[:, 2 * total - total // 2 :] / cells
    g = dot_nn(jnp.concatenate([folded[0:own], folded[own:]], axis=1), inv)
    start = pl.multiple_of(where_ref[0], own)
    for h, (orb_ref, stat) in enumerate(((mine_ref, stat_m), (other_ref, stat_o))):
        for z in range(planes):
            at = slice(z * half, (z + 1) * half)
            source = stat[natoms + planes + z : natoms + planes + z + 1, :] * orb_ref[pl.ds(start, own), at]
            r_ref[z * own : (z + 1) * own, h * half : (h + 1) * half] = dot_nn(g, orb_ref[:, at]) - source
    pc = inner_partials(r_ref, (stat_m, stat_o), w_ref, own, natoms)
    pc_ref[...] = pc
    pack_edges(where_ref, r_ref, pc, up_ref, down_ref, own)


def first_body(
    where_ref, v_ref, pc_ref, lo_ref, hi_ref, stat_m, stat_o, w_ref, coup_ref, en_ref,
    f_ref, up_ref, down_ref, out_pc_ref, *, own, natoms, cols,
):
    def emit(at, block):
        f_ref[:, at] = block

    apply_shift(emit, v_ref, pc_ref, lo_ref, hi_ref, (stat_m, stat_o), w_ref, coup_ref, en_ref, cols)
    pc = inner_partials(f_ref, (stat_m, stat_o), w_ref, own, natoms)
    out_pc_ref[...] = pc
    pack_edges(where_ref, f_ref, pc, up_ref, down_ref, own)


def target_body(
    freq_ref, v_ref, pc_ref, lo_ref, hi_ref, stat_m, stat_o, w_ref, coup_ref, en_ref, r_ref, mine_ref, other_ref,
    t_ref, out_ref, *, own, planes, cols,
):
    square = freq_ref[0] * freq_ref[0]

    def emit(at, block):
        t_ref[:, at] = block + square * r_ref[:, at]

    apply_shift(emit, v_ref, pc_ref, lo_ref, hi_ref, (stat_m, stat_o), w_ref, coup_ref, en_ref, cols)
    half = stat_m.shape[1]
    total = mine_ref.shape[0]
    corr = jnp.zeros((own, total), f32)
    for h, orb_ref in enumerate((mine_ref, other_ref)):
        for z in range(planes):
            block = t_ref[z * own : (z + 1) * own, h * half : (h + 1) * half]
            corr = corr + dot_nt(block, orb_ref[:, z * half : (z + 1) * half])
    rr = orbital_row_sums([b * b for b in lane_blocks(r_ref, cols)], own)
    ff = orbital_row_sums([b * b for b in lane_blocks(v_ref, cols)], own)
    lanes = out_ref.shape[1]
    lane = lax.broadcasted_iota(jnp.int32, (own, lanes), 1)
    spread = jnp.concatenate([corr, jnp.zeros((own, lanes - total), f32)], axis=1)
    out_ref[...] = jnp.where(lane == total, rr, jnp.where(lane == total + 1, ff, spread))


def residual_body(
    where_ref, freq_ref, sums_ref, inv_ref, r_ref, t_ref, mine_ref, other_ref, stat_m, stat_o, w_ref,
    out_ref, up_ref, down_ref, pc_ref, *, own, planes, natoms, cells,
):
    half = stat_m.shape[1]
    total = mine_ref.shape[0]
    square = freq_ref[0] * freq_ref[0]
    g = dot_nn(sums_ref[:, 0:total] / cells, inv_ref[...])
    rr, ff = sums_ref[:, total : total + 1], sums_ref[:, total + 1 : total + 2]
    step = rr / (ff + square * rr)
    for h, orb_ref in enumerate((mine_ref, other_ref)):
        for z in range(planes):
            rows, at = slice(z * own, (z + 1) * own), slice(h * half, (h + 1) * half)
            image = t_ref[rows, at] - dot_nn(g, orb_ref[:, z * half : (z + 1) * half])
            out_ref[rows, at] = r_ref[rows, at] - step * image
    pc = inner_partials(out_ref, (stat_m, stat_o), w_ref, own, natoms)
    pc_ref[...] = pc
    pack_edges(where_ref, out_ref, pc, up_ref, down_ref, own)


def last_body(
    v_ref, pc_ref, lo_ref, hi_ref, stat_m, stat_o, w_ref, coup_ref, en_ref, r_ref, f_ref, u_ref, out_ref, *, own, cols
):
    def emit(at, block):
        u_ref[:, at] = block

    apply_shift(emit, v_ref, pc_ref, lo_ref, hi_ref, (stat_m, stat_o), w_ref, coup_ref, en_ref, cols)
    r1, r0, u1, u0 = (lane_blocks(ref, cols) for ref in (v_ref, r_ref, u_ref, f_ref))
    values = [
        orbital_row_sums([a * b for a, b in zip(x, y)], own) for x, y in ((r1, r1), (u1, u1), (u1, u0), (r1, r0))
    ]
    lanes = out_ref.shape[1]
    lane = lax.broadcasted_iota(jnp.int32, (own, lanes), 1)
    row = lax.broadcasted_iota(jnp.int32, (own, lanes), 0)
    placed = sum(jnp.where(lane == own * s + row, value, 0.0) for s, value in enumerate(values))
    out_ref[...] = jnp.sum(placed, axis=0, keepdims=True)


def response_body(
    where_ref, freq_ref, sums_ref, lines_ref, f_ref, u_ref, mine_ref, other_ref, out_ref, swap_ref, dens_ref, *, own, planes
):
    total = mine_ref.shape[0]
    half = f_ref.shape[1] // 2
    square = freq_ref[0] * freq_ref[0]
    rr0, ff = sums_ref[:, total : total + 1], sums_ref[:, total + 1 : total + 2]
    line = lines_ref[...]
    lanes = line.shape[1]
    lane = lax.broadcasted_iota(jnp.int32, (own, lanes), 1)
    row = lax.broadcasted_iota(jnp.int32, (own, lanes), 0)
    rr1, uu, uf, rx = (
        jnp.sum(jnp.where(lane == own * s + row, line, 0.0), axis=1, keepdims=True) for s in range(4)
    )
    step0 = rr0 / (ff + square * rr0)
    beta = rr1 / rr0
    curvature = uu + 2.0 * beta * uf + beta * beta * ff + square * (rr1 + 2.0 * beta * rx + beta * beta * rr0)
    step1 = rr1 / curvature
    start = pl.multiple_of(where_ref[0], own)
    swap_ref[own:, :] = jnp.zeros((swap_ref.shape[0] - own, swap_ref.shape[1]), f32)
    for h, orb_ref in enumerate((mine_ref, other_ref)):
        for z in range(planes):
            rows, at = slice(z * own, (z + 1) * own), slice(h * half, (h + 1) * half)
            to = slice(z * half, (z + 1) * half)
            response = (step0 + step1 * beta) * f_ref[rows, at] + step1 * u_ref[rows, at]
            dens = jnp.sum(orb_ref[pl.ds(start, own), to] * response, axis=0, keepdims=True)
            if h == 0:
                out_ref[:, to] = response
                dens_ref[:, to] = dens
            else:
                swap_ref[0:own, to] = response
                swap_ref[own : own + 1, to] = dens


def copy_for_each(array, axis):
    copies = jnp.broadcast_to(array, (lax.axis_size(axis), *array.shape))
    return lax.all_to_all(copies, axis, split_axis=0, concat_axis=0, tiled=True)


def swap_cores(array):
    return lax.ppermute(array, "pen", [(0, 1), (1, 0)])


def turn(slab):
    return (slab + slab // NEAR) % 2


def place(slab, part):
    return 2 * slab + (part + turn(slab)) % 2


def summed(array):
    count = lax.axis_size("slab")
    runs = [[place(i + j, part) for j in range(NEAR)] for part in range(2) for i in range(0, count, NEAR)]
    across = [[place(i + j, part) for i in range(0, count, NEAR)] for part in range(2) for j in range(NEAR)]
    array = lax.psum(array, ("slab", "pen"), axis_index_groups=runs)
    return lax.psum(array, ("slab", "pen"), axis_index_groups=across)


def from_neighbours(up, down):
    count = lax.axis_size("slab")
    ring = [(place(i, part), place((i + 1) % count, part)) for i in range(count) for part in range(2)]
    axes = ("slab", "pen")
    return lax.ppermute(up, axes, ring), lax.ppermute(down, axes, [(b, a) for a, b in ring])


def plane_weights(atom_planes, profiles, planes, depth_total):
    span_size = profiles.shape[1]
    covered = (atom_planes[:, None] + jnp.arange(span_size, dtype=jnp.int32)[None, :]) % depth_total
    matches = (covered[None, :, :] == planes[:, None, None]).astype(jnp.float32)
    return jnp.sum(profiles[None, :, :] * matches, axis=2)


def on_device(
    orbitals, energies, frequency, local_potential, perturbation, projectors, profiles, couplings, atom_planes
):
    chip_count, planes, row_count, cols = orbitals.shape
    natoms = projectors.shape[0]
    half = row_count * cols
    slabs = lax.axis_size("slab")
    assert lax.axis_size("pen") == 2 and slabs > 2
    assert profiles.shape[1] == planes + 1
    depth_total = planes * slabs
    cells = float(depth_total * 2 * half)
    own = chip_count // 2
    slab = lax.axis_index("slab")
    core = (lax.axis_index("pen") + turn(slab)) % 2
    crossings = [(turn(slab) + turn((slab + step) % slabs)) % 2 for step in (1, slabs - 1)]
    first_plane = slab * planes
    weights = plane_weights(atom_planes, profiles, first_plane + jnp.arange(planes, dtype=jnp.int32), depth_total)
    where = jnp.stack([lax.axis_index("orb") * chip_count + core * own, core, *crossings]).astype(jnp.int32)
    own_energies = lax.dynamic_slice(energies, (core * own,), (own,)).reshape(own, 1)
    coup = couplings.reshape(1, natoms)

    stat_m = jnp.concatenate(
        [a.reshape(-1, half) for a in (projectors, local_potential, perturbation)], axis=0
    )
    stat_o = swap_cores(stat_m)
    mine = copy_for_each(orbitals.reshape(chip_count, planes * half), "orb").reshape(-1, planes * half)
    other = swap_cores(mine)
    total = mine.shape[0]
    stats = (stat_m, stat_o)
    field, edge, part = (planes * own, 2 * half), (own, 2 * half + natoms), (own, natoms)

    (gram_part,) = call(
        functools.partial(gram_body, own=own, planes=planes, natoms=natoms),
        (where, mine, other, *stats), "svvkk", [(total // 4, 2 * total)],
    )
    gram_sum = summed(gram_part)
    gram_other = swap_cores(gram_sum)
    r0, up, down, pc, inv = call(
        functools.partial(source_body, own=own, planes=planes, natoms=natoms, cells=cells),
        (where, gram_sum, gram_other, mine, other, *stats, weights), "skkvvkkk",
        [field, edge, edge, part, (total, total)],
    )
    lo, hi = from_neighbours(up, down)
    first, up, down, first_pc = call(
        functools.partial(first_body, own=own, natoms=natoms, cols=cols),
        (where, r0, pc, lo, hi, *stats, weights, coup, own_energies), "skkkkkkkkk", [field, edge, edge, part],
    )
    lo, hi = from_neighbours(up, down)
    target, sums_part = call(
        functools.partial(target_body, own=own, planes=planes, cols=cols),
        (frequency, first, first_pc, lo, hi, *stats, weights, coup, own_energies, r0, mine, other), "skkkkkkkkkkvv",
        [field, (own, 2 * total)],
    )
    sums = summed(sums_part)
    r1, up, down, pc = call(
        functools.partial(residual_body, own=own, planes=planes, natoms=natoms, cells=cells),
        (where, frequency, sums, inv, r0, target, mine, other, *stats, weights), "sskkkkvvkkk", [field, edge, edge, part],
    )
    lo, hi = from_neighbours(up, down)
    last, lines = call(
        functools.partial(last_body, own=own, cols=cols),
        (r1, pc, lo, hi, *stats, weights, coup, own_energies, r0, first), "kkkkkkkkkkk",
        [field, (1, 2 * total)],
    )
    lines = summed(lines)
    response, to_other, dens = call(
        functools.partial(response_body, own=own, planes=planes),
        (where, frequency, sums, lines, first, last, mine, other), "sskkkkvv",
        [(own, planes * half), (2 * own, planes * half), (1, planes * half)],
    )
    got = swap_cores(to_other)
    theirs = got[0:own]
    low, high = jnp.where(core == 0, response, theirs), jnp.where(core == 0, theirs, response)
    response_real = jnp.concatenate([low, high], axis=0).reshape(orbitals.shape)
    dens = (dens + got[own : own + 1]).reshape(planes, half)
    density = copy_for_each(dens, "orb").sum(axis=0) * (4.0 / NOCC)
    return response_real, density.reshape(planes, row_count, cols)


def solution(mesh):
    in_specs = (
        P(("parts", "orb"), "slab", "pen", None),
        P(("parts", "orb")),
        P("parts"),
        P("slab", "pen", None),
        P("slab", "pen", None),
        P(None, "pen", None),
        P(),
        P(),
        P(),
    )
    out_specs = (P(("parts", "orb"), "slab", "pen", None), P(("parts", "slab"), "pen", None))
    return jax.shard_map(on_device, mesh=mesh, in_specs=in_specs, out_specs=out_specs, check_vma=False)
```

```python
import functools

import jax
import jax.numpy as jnp
from jax import lax
from jax.experimental import pallas as pl
from jax.experimental.pallas import tpu as pltpu
from jax.sharding import PartitionSpec as P

NOCC = 64
NEAR = 4

kinetic_scale = 0.125
three_passes = lax.Precision.HIGH
f32 = jnp.float32
VMEM = pl.BlockSpec(memory_space=pltpu.VMEM)
SMEM = pl.BlockSpec(memory_space=pltpu.SMEM)


def dot_nn(a, b):
    return lax.dot_general(a, b, (((1,), (0,)), ((), ())), precision=three_passes, preferred_element_type=f32)


def dot_nt(a, b):
    return lax.dot_general(a, b, (((1,), (1,)), ((), ())), precision=three_passes, preferred_element_type=f32)


def call(body, args, kinds, outs):
    late = [pltpu.VMEM(a.shape, f32) for a, k in zip(args, kinds, strict=True) if k == "h"]
    args = [pltpu.with_memory_space_constraint(a, pltpu.VMEM) if k == "k" else a for a, k in zip(args, kinds, strict=True)]
    return pl.pallas_call(
        body,
        in_specs=[SMEM if k == "s" else pl.BlockSpec(memory_space=pl.ANY) if k == "h" else VMEM for k in kinds],
        out_specs=[VMEM] * len(outs),
        out_shape=[pltpu.VMEM(s, f32) for s in outs],
        scratch_shapes=[*late, pltpu.SemaphoreType.DMA((len(late),))] if late else [],
    )(*args)


def copies(pairs, sems):
    return [pltpu.make_async_copy(a, b, sems.at[i]) for i, (a, b) in enumerate(pairs)]


def orbital_row_sums(products, own):
    total = functools.reduce(jnp.add, products)
    folded = functools.reduce(jnp.add, [total[i : i + own] for i in range(0, total.shape[0], own)])
    return jnp.sum(folded, axis=1, keepdims=True)


def lane_blocks(ref, cols):
    return [ref[:, i : i + cols] for i in range(0, ref.shape[1], cols)]


def inner_partials(v_ref, stat_refs, w_ref, own, natoms):
    half = stat_refs[0].shape[1]
    sums = sum(
        dot_nt(v_ref[:, h * half : (h + 1) * half], stat_refs[h][0:natoms, :]) for h in range(2)
    )
    planes = w_ref.shape[0] - 1
    return sum(sums[z * own : (z + 1) * own] * w_ref[z : z + 1, :] for z in range(planes))


def pack_edges(where_ref, v_ref, pc, up_ref, down_ref, own):
    width = v_ref.shape[1]
    half = width // 2
    for ref, edge, crossing in (
        (up_ref, v_ref[v_ref.shape[0] - own :, :], where_ref[2] == 1),
        (down_ref, v_ref[0:own, :], where_ref[3] == 1),
    ):
        ref[:, 0:half] = jnp.where(crossing, edge[:, half:], edge[:, 0:half])
        ref[:, half:width] = jnp.where(crossing, edge[:, 0:half], edge[:, half:])
        ref[:, width:] = pc


def apply_shift(emit, v_ref, pc_ref, lo_ref, hi_ref, stat_refs, w_ref, en_ref, cols):
    own = lo_ref.shape[0]
    planes, natoms = w_ref.shape[0] - 1, w_ref.shape[1]
    width = v_ref.shape[1]
    half = width // 2
    c = w_ref[planes : planes + 1, :] * (pc_ref[...] + lo_ref[:, width:] + hi_ref[:, width:])
    spread = jnp.concatenate([c * w_ref[z : z + 1, :] for z in range(planes)], axis=0)
    shift = jnp.concatenate([6.0 * kinetic_scale - en_ref[...]] * planes, axis=0)
    blocks = width // cols
    for k in range(blocks):
        at = slice(k * cols, (k + 1) * cols)
        stat = stat_refs[k * cols // half]
        inside = (k * cols) % half
        nonlocal_term = dot_nn(spread, stat[0:natoms, inside : inside + cols])
        v = v_ref[:, at]
        after, before = (k + 1) % blocks, (k - 1) % blocks
        beside = v_ref[:, after * cols : (after + 1) * cols] + v_ref[:, before * cols : (before + 1) * cols]
        beside = beside + jnp.concatenate([lo_ref[:, at], v_ref[0 : own * (planes - 1), at]], axis=0)
        beside = beside + jnp.concatenate([v_ref[own:, at], hi_ref[:, at]], axis=0)
        beside = beside + pltpu.roll(v, 1, 1) + pltpu.roll(v, cols - 1, 1)
        local = jnp.concatenate(
            [
                jnp.broadcast_to(stat[natoms + z : natoms + z + 1, inside : inside + cols], (own, cols))
                for z in range(planes)
            ],
            axis=0,
        )
        emit(at, (local + shift) * v - kinetic_scale * beside + nonlocal_term)


def gram_body(where_ref, mine_ref, other_ref, stat_m, stat_o, out_ref, *, own, planes, natoms):
    half = stat_m.shape[1]
    total = mine_ref.shape[0]
    span, quarter = total // 2, total // 4
    rows = pl.ds(pl.multiple_of(where_ref[1] * span, span), span)
    start = pl.multiple_of(where_ref[0], own)
    sums = jnp.zeros((span + own, total), f32)
    for orb_ref, stat in ((mine_ref, stat_m), (other_ref, stat_o)):
        for z in range(planes):
            at = slice(z * half, (z + 1) * half)
            source = stat[natoms + planes + z : natoms + planes + z + 1, :] * orb_ref[pl.ds(start, own), at]
            sums = sums + dot_nt(jnp.concatenate([orb_ref[rows, at], source], axis=0), orb_ref[:, at])
    gram, corr = sums[0:span], sums[span:]
    twice = jnp.concatenate([gram, gram], axis=1)
    ahead = jnp.where(where_ref[1] == 0, twice[:, 0:total], twice[:, span : span + total])
    out_ref[...] = jnp.concatenate(
        [
            ahead[0:quarter, 0 : 3 * quarter],
            ahead[quarter:, quarter:],
            jnp.concatenate([corr[:, 0:span], corr[:, span:]], axis=0),
        ],
        axis=1,
    )


def gram_from(low, high):
    quarter = low.shape[0]
    blocks = [
        [part[:, i + d * quarter : i + (d + 1) * quarter] * (1.0 if d == 1 else 0.5) for d in range(3)]
        + [jnp.zeros((quarter, quarter), f32)]
        for part in (low, high)
        for i in (0, 3 * quarter)
    ]
    upper = jnp.concatenate(
        [jnp.concatenate([blocks[j][(k - j) % 4] for k in range(4)], axis=1) for j in range(4)], axis=0
    )
    return upper + upper.T


def inverse_of(gram):
    n = gram.shape[0]
    eye = (lax.broadcasted_iota(jnp.int32, (n, n), 0) == lax.broadcasted_iota(jnp.int32, (n, n), 1)).astype(f32)
    work = jnp.concatenate([gram, eye], axis=1)
    tiles = [work[i : i + 8] for i in range(0, n, 8)]
    sub = lax.broadcasted_iota(jnp.int32, (8, 2 * n), 0)
    for k in range(0, n, 2):
        t, r = divmod(k, 8)
        row0, row1 = tiles[t][r : r + 1, :], tiles[t][r + 1 : r + 2, :]
        a, b, d = row0[:, k : k + 1], row0[:, k + 1 : k + 2], row1[:, k + 1 : k + 2]
        det = a * d - b * b
        over = 1.0 / det
        x0 = row0 * (d * over) - row1 * (b * over)
        x1 = row1 * (a * over) - row0 * (b * over)
        for i in range(t, n // 8):
            step = tiles[i] - tiles[i][:, k : k + 1] * x0 - tiles[i][:, k + 1 : k + 2] * x1
            if i == t:
                first = row0 * lax.rsqrt(a)
                second = (row1 - row0 * (b / a)) * lax.rsqrt(det / a)
                kept = jnp.where(sub == r, first, jnp.where(sub == r + 1, second, tiles[i]))
                step = jnp.where(sub > r + 1, step, kept)
            tiles[i] = step
    lower_inverse = jnp.concatenate(tiles, axis=0)[:, n:]
    inv = lax.dot_general(
        lower_inverse, lower_inverse, (((0,), (0,)), ((), ())), precision=three_passes, preferred_element_type=f32
    )
    return 2.0 * inv - dot_nn(dot_nn(inv, gram), inv)


def source_body(
    where_ref, sums_ref, swapped_ref, mine_hbm, other_hbm, stat_m, stat_o, w_ref,
    r_ref, down_ref, up_ref, pc_ref, inv_ref, own_ref, mine_ref, other_ref, sems, *, own, planes, natoms, cells,
):
    arriving = copies([(mine_hbm, mine_ref), (other_hbm, other_ref)], sems)
    for copy in arriving:
        copy.start()
    half = stat_m.shape[1]
    total = mine_ref.shape[0]
    ours, theirs = sums_ref[...], swapped_ref[...]
    first = where_ref[1] == 0
    gram = gram_from(jnp.where(first, ours, theirs), jnp.where(first, theirs, ours)) / cells
    inv = inverse_of(gram)
    inv_ref[...] = inv
    folded = ours[:, 2 * total - total // 2 :] / cells
    g = dot_nn(jnp.concatenate([folded[0:own], folded[own:]], axis=1), inv)
    start = pl.multiple_of(where_ref[0], own)
    for copy in arriving:
        copy.wait()
    for h, (orb_ref, stat) in enumerate(((mine_ref, stat_m), (other_ref, stat_o))):
        for z in range(planes):
            at = slice(z * half, (z + 1) * half)
            mine = orb_ref[pl.ds(start, own), at]
            source = stat[natoms + planes + z : natoms + planes + z + 1, :] * mine
            own_ref[z * own : (z + 1) * own, h * half : (h + 1) * half] = mine
            r_ref[z * own : (z + 1) * own, h * half : (h + 1) * half] = dot_nn(g, orb_ref[:, at]) - source
    pc = inner_partials(r_ref, (stat_m, stat_o), w_ref, own, natoms)
    pc_ref[...] = pc
    pack_edges(where_ref, r_ref, pc, up_ref, down_ref, own)


def first_body(
    where_ref, v_ref, pc_ref, lo_ref, hi_ref, stat_m, stat_o, w_ref, en_ref,
    f_ref, down_ref, up_ref, out_pc_ref, *, own, natoms, cols,
):
    def emit(at, block):
        f_ref[:, at] = block

    apply_shift(emit, v_ref, pc_ref, lo_ref, hi_ref, (stat_m, stat_o), w_ref, en_ref, cols)
    pc = inner_partials(f_ref, (stat_m, stat_o), w_ref, own, natoms)
    out_pc_ref[...] = pc
    pack_edges(where_ref, f_ref, pc, up_ref, down_ref, own)


def target_body(
    freq_ref, v_ref, pc_ref, lo_ref, hi_ref, stat_m, stat_o, w_ref, en_ref, r_ref, mine_hbm, other_hbm,
    t_ref, out_ref, mine_ref, other_ref, sems, *, own, planes, cols,
):
    arriving = copies([(mine_hbm, mine_ref), (other_hbm, other_ref)], sems)
    for copy in arriving:
        copy.start()
    square = freq_ref[0] * freq_ref[0]

    def emit(at, block):
        t_ref[:, at] = block + square * r_ref[:, at]

    apply_shift(emit, v_ref, pc_ref, lo_ref, hi_ref, (stat_m, stat_o), w_ref, en_ref, cols)
    half = stat_m.shape[1]
    total = mine_ref.shape[0]
    corr = jnp.zeros((own, total), f32)
    for copy in arriving:
        copy.wait()
    for h, orb_ref in enumerate((mine_ref, other_ref)):
        for z in range(planes):
            block = t_ref[z * own : (z + 1) * own, h * half : (h + 1) * half]
            corr = corr + dot_nt(block, orb_ref[:, z * half : (z + 1) * half])
    rr = orbital_row_sums([b * b for b in lane_blocks(r_ref, cols)], own)
    ff = orbital_row_sums([b * b for b in lane_blocks(v_ref, cols)], own)
    lanes = out_ref.shape[1]
    lane = lax.broadcasted_iota(jnp.int32, (own, lanes), 1)
    spread = jnp.concatenate([corr, jnp.zeros((own, lanes - total), f32)], axis=1)
    out_ref[...] = jnp.where(lane == total, rr, jnp.where(lane == total + 1, ff, spread))


def residual_body(
    where_ref, freq_ref, sums_ref, inv_ref, r_ref, t_ref, mine_ref, other_ref, stat_m, stat_o, w_ref,
    out_ref, down_ref, up_ref, pc_ref, *, own, planes, natoms, cells,
):
    half = stat_m.shape[1]
    total = mine_ref.shape[0]
    square = freq_ref[0] * freq_ref[0]
    g = dot_nn(sums_ref[:, 0:total] / cells, inv_ref[...])
    rr, ff = sums_ref[:, total : total + 1], sums_ref[:, total + 1 : total + 2]
    step = rr / (ff + square * rr)
    for h, orb_ref in enumerate((mine_ref, other_ref)):
        for z in range(planes):
            rows, at = slice(z * own, (z + 1) * own), slice(h * half, (h + 1) * half)
            image = t_ref[rows, at] - dot_nn(g, orb_ref[:, z * half : (z + 1) * half])
            out_ref[rows, at] = r_ref[rows, at] - step * image
    pc = inner_partials(out_ref, (stat_m, stat_o), w_ref, own, natoms)
    pc_ref[...] = pc
    pack_edges(where_ref, out_ref, pc, up_ref, down_ref, own)


def last_body(
    v_ref, pc_ref, lo_ref, hi_ref, stat_m, stat_o, w_ref, en_ref, r_ref, f_ref, u_ref, out_ref, *, own, cols
):
    def emit(at, block):
        u_ref[:, at] = block

    apply_shift(emit, v_ref, pc_ref, lo_ref, hi_ref, (stat_m, stat_o), w_ref, en_ref, cols)
    r1, r0, u1, u0 = (lane_blocks(ref, cols) for ref in (v_ref, r_ref, u_ref, f_ref))
    values = [
        orbital_row_sums([a * b for a, b in zip(x, y)], own) for x, y in ((r1, r1), (u1, u1), (u1, u0), (r1, r0))
    ]
    lanes = out_ref.shape[1]
    lane = lax.broadcasted_iota(jnp.int32, (own, lanes), 1)
    row = lax.broadcasted_iota(jnp.int32, (own, lanes), 0)
    placed = sum(jnp.where(lane == own * s + row, value, 0.0) for s, value in enumerate(values))
    out_ref[...] = jnp.sum(placed, axis=0, keepdims=True)


def response_body(
    freq_ref, sums_ref, lines_ref, f_ref, u_ref, own_ref, out_ref, swap_ref, dens_ref, *, own, planes
):
    total = sums_ref.shape[1] // 2
    half = f_ref.shape[1] // 2
    square = freq_ref[0] * freq_ref[0]
    rr0, ff = sums_ref[:, total : total + 1], sums_ref[:, total + 1 : total + 2]
    line = lines_ref[...]
    lanes = line.shape[1]
    lane = lax.broadcasted_iota(jnp.int32, (own, lanes), 1)
    row = lax.broadcasted_iota(jnp.int32, (own, lanes), 0)
    rr1, uu, uf, rx = (
        jnp.sum(jnp.where(lane == own * s + row, line, 0.0), axis=1, keepdims=True) for s in range(4)
    )
    step0 = rr0 / (ff + square * rr0)
    beta = rr1 / rr0
    curvature = uu + 2.0 * beta * uf + beta * beta * ff + square * (rr1 + 2.0 * beta * rx + beta * beta * rr0)
    step1 = rr1 / curvature
    swap_ref[own:, :] = jnp.zeros((swap_ref.shape[0] - own, swap_ref.shape[1]), f32)
    for h in range(2):
        for z in range(planes):
            rows, at = slice(z * own, (z + 1) * own), slice(h * half, (h + 1) * half)
            to = slice(z * half, (z + 1) * half)
            response = (step0 + step1 * beta) * f_ref[rows, at] + step1 * u_ref[rows, at]
            dens = jnp.sum(own_ref[rows, at] * response, axis=0, keepdims=True)
            if h == 0:
                out_ref[:, to] = response
                dens_ref[:, to] = dens
            else:
                swap_ref[0:own, to] = response
                swap_ref[own : own + 1, to] = dens


def copy_for_each(array, axis):
    copies = jnp.broadcast_to(array, (lax.axis_size(axis), *array.shape))
    return lax.all_to_all(copies, axis, split_axis=0, concat_axis=0, tiled=True)


def swap_cores(array):
    return lax.ppermute(array, "pen", [(0, 1), (1, 0)])


def turn(slab):
    return (slab + slab // NEAR) % 2


def place(slab, part):
    return 2 * slab + (part + turn(slab)) % 2


def summed(array):
    count = lax.axis_size("slab")
    runs = [[place(i + j, part) for j in range(NEAR)] for part in range(2) for i in range(0, count, NEAR)]
    across = [[place(i + j, part) for i in range(0, count, NEAR)] for part in range(2) for j in range(NEAR)]
    array = lax.psum(array, ("slab", "pen"), axis_index_groups=runs)
    return lax.psum(array, ("slab", "pen"), axis_index_groups=across)


def from_neighbours(up, down):
    count = lax.axis_size("slab")
    ring = [(place(i, part), place((i + 1) % count, part)) for i in range(count) for part in range(2)]
    axes = ("slab", "pen")
    hi = lax.ppermute(down, axes, [(b, a) for a, b in ring])
    return lax.ppermute(up, axes, ring), hi


def plane_weights(atom_planes, profiles, planes, depth_total):
    span_size = profiles.shape[1]
    covered = (atom_planes[:, None] + jnp.arange(span_size, dtype=jnp.int32)[None, :]) % depth_total
    matches = (covered[None, :, :] == planes[:, None, None]).astype(jnp.float32)
    return jnp.sum(profiles[None, :, :] * matches, axis=2)


def on_device(
    orbitals, energies, frequency, local_potential, perturbation, projectors, profiles, couplings, atom_planes
):
    chip_count, planes, row_count, cols = orbitals.shape
    natoms = projectors.shape[0]
    half = row_count * cols
    slabs = lax.axis_size("slab")
    assert lax.axis_size("pen") == 2 and slabs > 2
    assert profiles.shape[1] == planes + 1
    depth_total = planes * slabs
    cells = float(depth_total * 2 * half)
    own = chip_count // 2
    slab = lax.axis_index("slab")
    core = (lax.axis_index("pen") + turn(slab)) % 2
    crossings = [(turn(slab) + turn((slab + step) % slabs)) % 2 for step in (1, slabs - 1)]
    first_plane = slab * planes
    weights = plane_weights(atom_planes, profiles, first_plane + jnp.arange(planes, dtype=jnp.int32), depth_total)
    where = jnp.stack([lax.axis_index("orb") * chip_count + core * own, core, *crossings]).astype(jnp.int32)
    own_energies = lax.dynamic_slice(energies, (core * own,), (own,)).reshape(own, 1)
    weights = jnp.concatenate([weights, couplings.reshape(1, natoms)], axis=0)

    stat_m = jnp.concatenate(
        [a.reshape(-1, half) for a in (projectors, local_potential, perturbation)], axis=0
    )
    stat_o = swap_cores(stat_m)
    mine = copy_for_each(orbitals.reshape(chip_count, planes * half), "orb").reshape(-1, planes * half)
    other = swap_cores(mine)
    total = mine.shape[0]
    stats = (stat_m, stat_o)
    field, edge, part = (planes * own, 2 * half), (own, 2 * half + natoms), (own, natoms)

    (gram_part,) = call(
        functools.partial(gram_body, own=own, planes=planes, natoms=natoms),
        (where, mine, other, *stats), "svvkk", [(total // 4, 2 * total)],
    )
    gram_sum = summed(gram_part)
    gram_other = swap_cores(gram_sum)
    r0, down, up, pc, inv, own_orbitals = call(
        functools.partial(source_body, own=own, planes=planes, natoms=natoms, cells=cells),
        (where, gram_sum, gram_other, mine, other, *stats, weights), "skkhhkkk",
        [field, edge, edge, part, (total, total), field],
    )
    lo, hi = from_neighbours(up, down)
    first, down, up, first_pc = call(
        functools.partial(first_body, own=own, natoms=natoms, cols=cols),
        (where, r0, pc, lo, hi, *stats, weights, own_energies), "skkkkkkkk", [field, edge, edge, part],
    )
    lo, hi = from_neighbours(up, down)
    target, sums_part = call(
        functools.partial(target_body, own=own, planes=planes, cols=cols),
        (frequency, first, first_pc, lo, hi, *stats, weights, own_energies, r0, mine, other), "skkkkkkkkkhh",
        [field, (own, 2 * total)],
    )
    sums = summed(sums_part)
    r1, down, up, pc = call(
        functools.partial(residual_body, own=own, planes=planes, natoms=natoms, cells=cells),
        (where, frequency, sums, inv, r0, target, mine, other, *stats, weights), "sskkkkvvkkk", [field, edge, edge, part],
    )
    lo, hi = from_neighbours(up, down)
    last, lines = call(
        functools.partial(last_body, own=own, cols=cols),
        (r1, pc, lo, hi, *stats, weights, own_energies, r0, first), "kkkkkkkkkk",
        [field, (1, 2 * total)],
    )
    lines = summed(lines)
    response, to_other, dens = call(
        functools.partial(response_body, own=own, planes=planes),
        (frequency, sums, lines, first, last, own_orbitals), "skkkkk",
        [(own, planes * half), (2 * own, planes * half), (1, planes * half)],
    )
    got = swap_cores(to_other)
    theirs = got[0:own]
    low, high = jnp.where(core == 0, response, theirs), jnp.where(core == 0, theirs, response)
    response_real = jnp.concatenate([low, high], axis=0).reshape(orbitals.shape)
    dens = (dens + got[own : own + 1]).reshape(planes, half)
    density = copy_for_each(dens, "orb").sum(axis=0) * (4.0 / NOCC)
    return response_real, density.reshape(planes, row_count, cols)


def solution(mesh):
    in_specs = (
        P(("parts", "orb"), "slab", "pen", None),
        P(("parts", "orb")),
        P("parts"),
        P("slab", "pen", None),
        P("slab", "pen", None),
        P(None, "pen", None),
        P(),
        P(),
        P(),
    )
    out_specs = (P(("parts", "orb"), "slab", "pen", None), P(("parts", "slab"), "pen", None))
    return jax.shard_map(on_device, mesh=mesh, in_specs=in_specs, out_specs=out_specs, check_vma=False)
```

```python
import functools

import jax
import jax.numpy as jnp
from jax import lax
from jax.experimental import pallas as pl
from jax.experimental.pallas import tpu as pltpu
from jax.sharding import PartitionSpec as P

NOCC = 64
NEAR = 4

kinetic_scale = 0.125
highest, three_passes = lax.Precision.HIGHEST, lax.Precision.HIGH
f32 = jnp.float32
VMEM = pl.BlockSpec(memory_space=pltpu.VMEM)
SMEM = pl.BlockSpec(memory_space=pltpu.SMEM)


def dot_nn(a, b, precision=highest):
    return lax.dot_general(a, b, (((1,), (0,)), ((), ())), precision=precision, preferred_element_type=f32)


def dot_nt(a, b, precision=highest):
    return lax.dot_general(a, b, (((1,), (1,)), ((), ())), precision=precision, preferred_element_type=f32)


def call(body, args, kinds, outs):
    late = [pltpu.VMEM(a.shape, f32) for a, k in zip(args, kinds, strict=True) if k == "h"]
    args = [pltpu.with_memory_space_constraint(a, pltpu.VMEM) if k == "k" else a for a, k in zip(args, kinds, strict=True)]
    return pl.pallas_call(
        body,
        in_specs=[SMEM if k == "s" else pl.BlockSpec(memory_space=pl.ANY) if k == "h" else VMEM for k in kinds],
        out_specs=[VMEM] * len(outs),
        out_shape=[pltpu.VMEM(s, f32) for s in outs],
        scratch_shapes=[*late, pltpu.SemaphoreType.DMA((len(late),))] if late else [],
    )(*args)


def copies(pairs, sems):
    return [pltpu.make_async_copy(a, b, sems.at[i]) for i, (a, b) in enumerate(pairs)]


def orbital_row_sums(products, own):
    total = functools.reduce(jnp.add, products)
    folded = functools.reduce(jnp.add, [total[i : i + own] for i in range(0, total.shape[0], own)])
    return jnp.sum(folded, axis=1, keepdims=True)


def lane_blocks(ref, cols):
    return [ref[:, i : i + cols] for i in range(0, ref.shape[1], cols)]


def inner_partials(v_ref, stat_refs, w_ref, own, natoms):
    half = stat_refs[0].shape[1]
    sums = sum(
        dot_nt(v_ref[:, h * half : (h + 1) * half], stat_refs[h][0:natoms, :], three_passes) for h in range(2)
    )
    planes = w_ref.shape[0] - 1
    return sum(sums[z * own : (z + 1) * own] * w_ref[z : z + 1, :] for z in range(planes))


def pack_edges(where_ref, v_ref, pc, even_ref, odd_ref, own):
    width = v_ref.shape[1]
    half = width // 2
    is_even = where_ref[4] == 0
    top, bottom = v_ref[v_ref.shape[0] - own :, :], v_ref[0:own, :]
    for ref, edge, crossing in (
        (even_ref, jnp.where(is_even, top, bottom), jnp.where(is_even, where_ref[2], where_ref[3]) == 1),
        (odd_ref, jnp.where(is_even, bottom, top), jnp.where(is_even, where_ref[3], where_ref[2]) == 1),
    ):
        ref[:, 0:half] = jnp.where(crossing, edge[:, half:], edge[:, 0:half])
        ref[:, half:width] = jnp.where(crossing, edge[:, 0:half], edge[:, half:])
        ref[:, width:] = pc


def apply_shift(emit, where_ref, v_ref, pc_ref, odd_ref, even_ref, stat_refs, w_ref, en_ref, cols):
    own = odd_ref.shape[0]
    is_even = where_ref[4] == 0
    planes, natoms = w_ref.shape[0] - 1, w_ref.shape[1]
    width = v_ref.shape[1]
    half = width // 2
    c = w_ref[planes : planes + 1, :] * (pc_ref[...] + odd_ref[:, width:] + even_ref[:, width:])
    spread = jnp.concatenate([c * w_ref[z : z + 1, :] for z in range(planes)], axis=0)
    shift = jnp.concatenate([6.0 * kinetic_scale - en_ref[...]] * planes, axis=0)
    blocks = width // cols
    for k in range(blocks):
        at = slice(k * cols, (k + 1) * cols)
        stat = stat_refs[k * cols // half]
        inside = (k * cols) % half
        odd, even = odd_ref[:, at], even_ref[:, at]
        nonlocal_term = dot_nn(spread, stat[0:natoms, inside : inside + cols], three_passes)
        v = v_ref[:, at]
        after, before = (k + 1) % blocks, (k - 1) % blocks
        beside = v_ref[:, after * cols : (after + 1) * cols] + v_ref[:, before * cols : (before + 1) * cols]
        beside = beside + jnp.concatenate([jnp.where(is_even, odd, even), v_ref[0 : own * (planes - 1), at]], axis=0)
        beside = beside + jnp.concatenate([v_ref[own:, at], jnp.where(is_even, even, odd)], axis=0)
        beside = beside + pltpu.roll(v, 1, 1) + pltpu.roll(v, cols - 1, 1)
        local = jnp.concatenate(
            [
                jnp.broadcast_to(stat[natoms + z : natoms + z + 1, inside : inside + cols], (own, cols))
                for z in range(planes)
            ],
            axis=0,
        )
        emit(at, (local + shift) * v - kinetic_scale * beside + nonlocal_term)


def gram_body(where_ref, mine_ref, other_ref, stat_m, stat_o, out_ref, *, own, planes, natoms):
    half = stat_m.shape[1]
    total = mine_ref.shape[0]
    span, quarter = total // 2, total // 4
    rows = pl.ds(pl.multiple_of(where_ref[1] * span, span), span)
    start = pl.multiple_of(where_ref[0], own)
    sums = jnp.zeros((span + own, total), f32)
    for orb_ref, stat in ((mine_ref, stat_m), (other_ref, stat_o)):
        for z in range(planes):
            at = slice(z * half, (z + 1) * half)
            source = stat[natoms + planes + z : natoms + planes + z + 1, :] * orb_ref[pl.ds(start, own), at]
            sums = sums + dot_nt(jnp.concatenate([orb_ref[rows, at], source], axis=0), orb_ref[:, at])
    gram, corr = sums[0:span], sums[span:]
    twice = jnp.concatenate([gram, gram], axis=1)
    ahead = jnp.where(where_ref[1] == 0, twice[:, 0:total], twice[:, span : span + total])
    out_ref[...] = jnp.concatenate(
        [
            ahead[0:quarter, 0 : 3 * quarter],
            ahead[quarter:, quarter:],
            jnp.concatenate([corr[:, 0:span], corr[:, span:]], axis=0),
        ],
        axis=1,
    )


def gram_from(low, high):
    quarter = low.shape[0]
    blocks = [
        [part[:, i + d * quarter : i + (d + 1) * quarter] * (1.0 if d == 1 else 0.5) for d in range(3)]
        + [jnp.zeros((quarter, quarter), f32)]
        for part in (low, high)
        for i in (0, 3 * quarter)
    ]
    upper = jnp.concatenate(
        [jnp.concatenate([blocks[j][(k - j) % 4] for k in range(4)], axis=1) for j in range(4)], axis=0
    )
    return upper + upper.T


def inverse_of(gram):
    n = gram.shape[0]
    eye = (lax.broadcasted_iota(jnp.int32, (n, n), 0) == lax.broadcasted_iota(jnp.int32, (n, n), 1)).astype(f32)
    work = jnp.concatenate([gram, eye], axis=1)
    tiles = [work[i : i + 8] for i in range(0, n, 8)]
    sub = lax.broadcasted_iota(jnp.int32, (8, 2 * n), 0)
    for k in range(0, n, 2):
        t, r = divmod(k, 8)
        row0, row1 = tiles[t][r : r + 1, :], tiles[t][r + 1 : r + 2, :]
        a, b, d = row0[:, k : k + 1], row0[:, k + 1 : k + 2], row1[:, k + 1 : k + 2]
        det = a * d - b * b
        over = 1.0 / det
        x0 = row0 * (d * over) - row1 * (b * over)
        x1 = row1 * (a * over) - row0 * (b * over)
        for i in range(t, n // 8):
            step = tiles[i] - tiles[i][:, k : k + 1] * x0 - tiles[i][:, k + 1 : k + 2] * x1
            if i == t:
                first = row0 * lax.rsqrt(a)
                second = (row1 - row0 * (b / a)) * lax.rsqrt(det / a)
                kept = jnp.where(sub == r, first, jnp.where(sub == r + 1, second, tiles[i]))
                step = jnp.where(sub > r + 1, step, kept)
            tiles[i] = step
    lower_inverse = jnp.concatenate(tiles, axis=0)[:, n:]
    inv = lax.dot_general(
        lower_inverse, lower_inverse, (((0,), (0,)), ((), ())), precision=highest, preferred_element_type=f32
    )
    return 2.0 * inv - dot_nn(dot_nn(inv, gram), inv)


def source_body(
    where_ref, sums_ref, swapped_ref, mine_hbm, other_hbm, stat_m, stat_o, w_ref,
    r_ref, even_edge, odd_edge, pc_ref, inv_ref, own_ref, mine_ref, other_ref, sems, *, own, planes, natoms, cells,
):
    arriving = copies([(mine_hbm, mine_ref), (other_hbm, other_ref)], sems)
    for copy in arriving:
        copy.start()
    half = stat_m.shape[1]
    total = mine_ref.shape[0]
    ours, theirs = sums_ref[...], swapped_ref[...]
    first = where_ref[1] == 0
    gram = gram_from(jnp.where(first, ours, theirs), jnp.where(first, theirs, ours)) / cells
    inv = inverse_of(gram)
    inv_ref[...] = inv
    folded = ours[:, 2 * total - total // 2 :] / cells
    g = dot_nn(jnp.concatenate([folded[0:own], folded[own:]], axis=1), inv)
    start = pl.multiple_of(where_ref[0], own)
    for copy in arriving:
        copy.wait()
    for h, (orb_ref, stat) in enumerate(((mine_ref, stat_m), (other_ref, stat_o))):
        for z in range(planes):
            at = slice(z * half, (z + 1) * half)
            mine = orb_ref[pl.ds(start, own), at]
            source = stat[natoms + planes + z : natoms + planes + z + 1, :] * mine
            own_ref[z * own : (z + 1) * own, h * half : (h + 1) * half] = mine
            r_ref[z * own : (z + 1) * own, h * half : (h + 1) * half] = dot_nn(g, orb_ref[:, at]) - source
    pc = inner_partials(r_ref, (stat_m, stat_o), w_ref, own, natoms)
    pc_ref[...] = pc
    pack_edges(where_ref, r_ref, pc, even_edge, odd_edge, own)


def first_body(
    where_ref, v_ref, pc_ref, odd_ref, even_ref, stat_m, stat_o, w_ref, en_ref,
    f_ref, even_edge, odd_edge, out_pc_ref, *, own, natoms, cols,
):
    def emit(at, block):
        f_ref[:, at] = block

    apply_shift(emit, where_ref, v_ref, pc_ref, odd_ref, even_ref, (stat_m, stat_o), w_ref, en_ref, cols)
    pc = inner_partials(f_ref, (stat_m, stat_o), w_ref, own, natoms)
    out_pc_ref[...] = pc
    pack_edges(where_ref, f_ref, pc, even_edge, odd_edge, own)


def target_body(
    where_ref, freq_ref, v_ref, pc_ref, odd_ref, even_ref, stat_m, stat_o, w_ref, en_ref, r_ref, mine_hbm, other_hbm,
    t_ref, out_ref, mine_ref, other_ref, sems, *, own, planes, cols,
):
    arriving = copies([(mine_hbm, mine_ref), (other_hbm, other_ref)], sems)
    for copy in arriving:
        copy.start()
    square = freq_ref[0] * freq_ref[0]

    def emit(at, block):
        t_ref[:, at] = block + square * r_ref[:, at]

    apply_shift(emit, where_ref, v_ref, pc_ref, odd_ref, even_ref, (stat_m, stat_o), w_ref, en_ref, cols)
    half = stat_m.shape[1]
    total = mine_ref.shape[0]
    corr = jnp.zeros((own, total), f32)
    for copy in arriving:
        copy.wait()
    for h, orb_ref in enumerate((mine_ref, other_ref)):
        for z in range(planes):
            block = t_ref[z * own : (z + 1) * own, h * half : (h + 1) * half]
            corr = corr + dot_nt(block, orb_ref[:, z * half : (z + 1) * half])
    rr = orbital_row_sums([b * b for b in lane_blocks(r_ref, cols)], own)
    ff = orbital_row_sums([b * b for b in lane_blocks(v_ref, cols)], own)
    lanes = out_ref.shape[1]
    lane = lax.broadcasted_iota(jnp.int32, (own, lanes), 1)
    spread = jnp.concatenate([corr, jnp.zeros((own, lanes - total), f32)], axis=1)
    out_ref[...] = jnp.where(lane == total, rr, jnp.where(lane == total + 1, ff, spread))


def residual_body(
    where_ref, freq_ref, sums_ref, inv_ref, r_ref, t_ref, mine_ref, other_ref, stat_m, stat_o, w_ref,
    out_ref, even_edge, odd_edge, pc_ref, *, own, planes, natoms, cells,
):
    half = stat_m.shape[1]
    total = mine_ref.shape[0]
    square = freq_ref[0] * freq_ref[0]
    g = dot_nn(sums_ref[:, 0:total] / cells, inv_ref[...])
    rr, ff = sums_ref[:, total : total + 1], sums_ref[:, total + 1 : total + 2]
    step = rr / (ff + square * rr)
    for h, orb_ref in enumerate((mine_ref, other_ref)):
        for z in range(planes):
            rows, at = slice(z * own, (z + 1) * own), slice(h * half, (h + 1) * half)
            image = t_ref[rows, at] - dot_nn(g, orb_ref[:, z * half : (z + 1) * half])
            out_ref[rows, at] = r_ref[rows, at] - step * image
    pc = inner_partials(out_ref, (stat_m, stat_o), w_ref, own, natoms)
    pc_ref[...] = pc
    pack_edges(where_ref, out_ref, pc, even_edge, odd_edge, own)


def last_body(
    where_ref, v_ref, pc_ref, odd_ref, even_ref, stat_m, stat_o, w_ref, en_ref, r_ref, f_ref, u_ref, out_ref, *, own, cols
):
    def emit(at, block):
        u_ref[:, at] = block

    apply_shift(emit, where_ref, v_ref, pc_ref, odd_ref, even_ref, (stat_m, stat_o), w_ref, en_ref, cols)
    r1, r0, u1, u0 = (lane_blocks(ref, cols) for ref in (v_ref, r_ref, u_ref, f_ref))
    values = [
        orbital_row_sums([a * b for a, b in zip(x, y)], own) for x, y in ((r1, r1), (u1, u1), (u1, u0), (r1, r0))
    ]
    lanes = out_ref.shape[1]
    lane = lax.broadcasted_iota(jnp.int32, (own, lanes), 1)
    row = lax.broadcasted_iota(jnp.int32, (own, lanes), 0)
    placed = sum(jnp.where(lane == own * s + row, value, 0.0) for s, value in enumerate(values))
    out_ref[...] = jnp.sum(placed, axis=0, keepdims=True)


def response_body(
    freq_ref, sums_ref, lines_ref, f_ref, u_ref, own_ref, out_ref, swap_ref, dens_ref, *, own, planes
):
    total = sums_ref.shape[1] // 2
    half = f_ref.shape[1] // 2
    square = freq_ref[0] * freq_ref[0]
    rr0, ff = sums_ref[:, total : total + 1], sums_ref[:, total + 1 : total + 2]
    line = lines_ref[...]
    lanes = line.shape[1]
    lane = lax.broadcasted_iota(jnp.int32, (own, lanes), 1)
    row = lax.broadcasted_iota(jnp.int32, (own, lanes), 0)
    rr1, uu, uf, rx = (
        jnp.sum(jnp.where(lane == own * s + row, line, 0.0), axis=1, keepdims=True) for s in range(4)
    )
    step0 = rr0 / (ff + square * rr0)
    beta = rr1 / rr0
    curvature = uu + 2.0 * beta * uf + beta * beta * ff + square * (rr1 + 2.0 * beta * rx + beta * beta * rr0)
    step1 = rr1 / curvature
    swap_ref[own:, :] = jnp.zeros((swap_ref.shape[0] - own, swap_ref.shape[1]), f32)
    for h in range(2):
        for z in range(planes):
            rows, at = slice(z * own, (z + 1) * own), slice(h * half, (h + 1) * half)
            to = slice(z * half, (z + 1) * half)
            response = (step0 + step1 * beta) * f_ref[rows, at] + step1 * u_ref[rows, at]
            dens = jnp.sum(own_ref[rows, at] * response, axis=0, keepdims=True)
            if h == 0:
                out_ref[:, to] = response
                dens_ref[:, to] = dens
            else:
                swap_ref[0:own, to] = response
                swap_ref[own : own + 1, to] = dens


def copy_for_each(array, axis):
    copies = jnp.broadcast_to(array, (lax.axis_size(axis), *array.shape))
    return lax.all_to_all(copies, axis, split_axis=0, concat_axis=0, tiled=True)


def swap_cores(array):
    return lax.ppermute(array, "pen", [(0, 1), (1, 0)])


def turn(slab):
    return (slab + slab // NEAR) % 2


def place(slab, part):
    return 2 * slab + (part + turn(slab)) % 2


def summed(array):
    count = lax.axis_size("slab")
    runs = [[place(i + j, part) for j in range(NEAR)] for part in range(2) for i in range(0, count, NEAR)]
    across = [[place(i + j, part) for i in range(0, count, NEAR)] for part in range(2) for j in range(NEAR)]
    array = lax.psum(array, ("slab", "pen"), axis_index_groups=runs)
    return lax.psum(array, ("slab", "pen"), axis_index_groups=across)


def from_neighbours(even_edge, odd_edge):
    count = lax.axis_size("slab")

    def pairs(first):
        both = [(i, (i + 1) % count) for i in range(first, count, 2)]
        return [(place(a, part), place(b, part)) for i, j in both for a, b in ((i, j), (j, i)) for part in range(2)]

    axes = ("slab", "pen")
    return lax.ppermute(odd_edge, axes, pairs(1)), lax.ppermute(even_edge, axes, pairs(0))


def plane_weights(atom_planes, profiles, planes, depth_total):
    span_size = profiles.shape[1]
    covered = (atom_planes[:, None] + jnp.arange(span_size, dtype=jnp.int32)[None, :]) % depth_total
    matches = (covered[None, :, :] == planes[:, None, None]).astype(jnp.float32)
    return jnp.sum(profiles[None, :, :] * matches, axis=2)


def on_device(
    orbitals, energies, frequency, local_potential, perturbation, projectors, profiles, couplings, atom_planes
):
    chip_count, planes, row_count, cols = orbitals.shape
    natoms = projectors.shape[0]
    half = row_count * cols
    slabs = lax.axis_size("slab")
    assert lax.axis_size("pen") == 2 and slabs > 2 and slabs % 2 == 0
    assert profiles.shape[1] == planes + 1
    depth_total = planes * slabs
    cells = float(depth_total * 2 * half)
    own = chip_count // 2
    slab = lax.axis_index("slab")
    core = (lax.axis_index("pen") + turn(slab)) % 2
    crossings = [(turn(slab) + turn((slab + step) % slabs)) % 2 for step in (1, slabs - 1)]
    first_plane = slab * planes
    weights = plane_weights(atom_planes, profiles, first_plane + jnp.arange(planes, dtype=jnp.int32), depth_total)
    where = jnp.stack([lax.axis_index("orb") * chip_count + core * own, core, *crossings, slab % 2]).astype(jnp.int32)
    own_energies = lax.dynamic_slice(energies, (core * own,), (own,)).reshape(own, 1)
    weights = jnp.concatenate([weights, couplings.reshape(1, natoms)], axis=0)

    stat_m = jnp.concatenate(
        [a.reshape(-1, half) for a in (projectors, local_potential, perturbation)], axis=0
    )
    stat_o = swap_cores(stat_m)
    mine = copy_for_each(orbitals.reshape(chip_count, planes * half), "orb").reshape(-1, planes * half)
    other = swap_cores(mine)
    total = mine.shape[0]
    stats = (stat_m, stat_o)
    field, edge, part = (planes * own, 2 * half), (own, 2 * half + natoms), (own, natoms)

    (gram_part,) = call(
        functools.partial(gram_body, own=own, planes=planes, natoms=natoms),
        (where, mine, other, *stats), "svvkk", [(total // 4, 2 * total)],
    )
    gram_sum = summed(gram_part)
    gram_other = swap_cores(gram_sum)
    r0, even, odd, pc, inv, own_orbitals = call(
        functools.partial(source_body, own=own, planes=planes, natoms=natoms, cells=cells),
        (where, gram_sum, gram_other, mine, other, *stats, weights), "skkhhkkk",
        [field, edge, edge, part, (total, total), field],
    )
    odd, even = from_neighbours(even, odd)
    first, even, odd, first_pc = call(
        functools.partial(first_body, own=own, natoms=natoms, cols=cols),
        (where, r0, pc, odd, even, *stats, weights, own_energies), "skkkkkkkk", [field, edge, edge, part],
    )
    odd, even = from_neighbours(even, odd)
    target, sums_part = call(
        functools.partial(target_body, own=own, planes=planes, cols=cols),
        (where, frequency, first, first_pc, odd, even, *stats, weights, own_energies, r0, mine, other), "sskkkkkkkkkhh",
        [field, (own, 2 * total)],
    )
    sums = summed(sums_part)
    r1, even, odd, pc = call(
        functools.partial(residual_body, own=own, planes=planes, natoms=natoms, cells=cells),
        (where, frequency, sums, inv, r0, target, mine, other, *stats, weights), "sskkkkvvkkk", [field, edge, edge, part],
    )
    odd, even = from_neighbours(even, odd)
    last, lines = call(
        functools.partial(last_body, own=own, cols=cols),
        (where, r1, pc, odd, even, *stats, weights, own_energies, r0, first), "skkkkkkkkkk",
        [field, (1, 2 * total)],
    )
    lines = summed(lines)
    response, to_other, dens = call(
        functools.partial(response_body, own=own, planes=planes),
        (frequency, sums, lines, first, last, own_orbitals), "skkkkk",
        [(own, planes * half), (2 * own, planes * half), (1, planes * half)],
    )
    got = swap_cores(to_other)
    theirs = got[0:own]
    low, high = jnp.where(core == 0, response, theirs), jnp.where(core == 0, theirs, response)
    response_real = jnp.concatenate([low, high], axis=0).reshape(orbitals.shape)
    dens = (dens + got[own : own + 1]).reshape(planes, half)
    density = copy_for_each(dens, "orb").sum(axis=0) * (4.0 / NOCC)
    return response_real, density.reshape(planes, row_count, cols)


def solution(mesh):
    in_specs = (
        P(("parts", "orb"), "slab", "pen", None),
        P(("parts", "orb")),
        P("parts"),
        P("slab", "pen", None),
        P("slab", "pen", None),
        P(None, "pen", None),
        P(),
        P(),
        P(),
    )
    out_specs = (P(("parts", "orb"), "slab", "pen", None), P(("parts", "slab"), "pen", None))
    return jax.shard_map(on_device, mesh=mesh, in_specs=in_specs, out_specs=out_specs, check_vma=False)
```

```python
import functools

import jax
import jax.numpy as jnp
from jax import lax
from jax.experimental import pallas as pl
from jax.experimental.pallas import tpu as pltpu
from jax.sharding import PartitionSpec as P

NOCC = 64
NEAR = 4

kinetic_scale = 0.125
highest, three_passes = lax.Precision.HIGHEST, lax.Precision.HIGH
f32 = jnp.float32
VMEM = pl.BlockSpec(memory_space=pltpu.VMEM)
SMEM = pl.BlockSpec(memory_space=pltpu.SMEM)


def dot_nn(a, b, precision=highest):
    return lax.dot_general(a, b, (((1,), (0,)), ((), ())), precision=precision, preferred_element_type=f32)


def dot_nt(a, b, precision=highest):
    return lax.dot_general(a, b, (((1,), (1,)), ((), ())), precision=precision, preferred_element_type=f32)


def call(body, args, kinds, outs):
    late = [pltpu.VMEM(a.shape, f32) for a, k in zip(args, kinds, strict=True) if k == "h"]
    args = [pltpu.with_memory_space_constraint(a, pltpu.VMEM) if k == "k" else a for a, k in zip(args, kinds, strict=True)]
    return pl.pallas_call(
        body,
        in_specs=[SMEM if k == "s" else pl.BlockSpec(memory_space=pl.ANY) if k == "h" else VMEM for k in kinds],
        out_specs=[VMEM] * len(outs),
        out_shape=[pltpu.VMEM(s, f32) for s in outs],
        scratch_shapes=[*late, pltpu.SemaphoreType.DMA((len(late),))] if late else [],
    )(*args)


def copies(pairs, sems):
    return [pltpu.make_async_copy(a, b, sems.at[i]) for i, (a, b) in enumerate(pairs)]


BELOW = 5


def flag(w_ref, row, shape):
    at = w_ref.shape[0] - BELOW + row
    return jnp.broadcast_to(w_ref[at : at + 1, 0:1], shape) > 0.5


def squared_frequency(w_ref):
    at = w_ref.shape[0] - BELOW + 1
    return w_ref[at : at + 1, 0:1]


def orbital_row_sums(products, own):
    total = functools.reduce(jnp.add, products)
    folded = functools.reduce(jnp.add, [total[i : i + own] for i in range(0, total.shape[0], own)])
    return jnp.sum(folded, axis=1, keepdims=True)


def lane_blocks(ref, cols):
    return [ref[:, i : i + cols] for i in range(0, ref.shape[1], cols)]


def inner_partials(v_ref, stat_refs, w_ref, own, natoms):
    half = stat_refs[0].shape[1]
    sums = sum(
        dot_nt(v_ref[:, h * half : (h + 1) * half], stat_refs[h][0:natoms, :], three_passes) for h in range(2)
    )
    planes = w_ref.shape[0] - BELOW
    return sum(sums[z * own : (z + 1) * own] * w_ref[z : z + 1, :] for z in range(planes))


def pack_edges(w_ref, v_ref, pc, even_ref, odd_ref, own):
    width = v_ref.shape[1]
    half = width // 2
    is_even = flag(w_ref, 2, (own, width))
    top, bottom = v_ref[v_ref.shape[0] - own :, :], v_ref[0:own, :]
    for ref, edge, row in ((even_ref, jnp.where(is_even, top, bottom), 3), (odd_ref, jnp.where(is_even, bottom, top), 4)):
        crossing = flag(w_ref, row, (own, half))
        ref[:, 0:half] = jnp.where(crossing, edge[:, half:], edge[:, 0:half])
        ref[:, half:width] = jnp.where(crossing, edge[:, 0:half], edge[:, half:])
        ref[:, width:] = pc


def apply_shift(emit, v_ref, pc_ref, odd_ref, even_ref, stat_refs, w_ref, en_ref, cols):
    own = odd_ref.shape[0]
    is_even = flag(w_ref, 2, (own, cols))
    planes, natoms = w_ref.shape[0] - BELOW, w_ref.shape[1]
    width = v_ref.shape[1]
    half = width // 2
    c = w_ref[planes : planes + 1, :] * (pc_ref[...] + odd_ref[:, width:] + even_ref[:, width:])
    spread = jnp.concatenate([c * w_ref[z : z + 1, :] for z in range(planes)], axis=0)
    shift = jnp.concatenate([6.0 * kinetic_scale - en_ref[...]] * planes, axis=0)
    blocks = width // cols
    for k in range(blocks):
        at = slice(k * cols, (k + 1) * cols)
        stat = stat_refs[k * cols // half]
        inside = (k * cols) % half
        odd, even = odd_ref[:, at], even_ref[:, at]
        nonlocal_term = dot_nn(spread, stat[0:natoms, inside : inside + cols], three_passes)
        v = v_ref[:, at]
        after, before = (k + 1) % blocks, (k - 1) % blocks
        beside = v_ref[:, after * cols : (after + 1) * cols] + v_ref[:, before * cols : (before + 1) * cols]
        beside = beside + jnp.concatenate([jnp.where(is_even, odd, even), v_ref[0 : own * (planes - 1), at]], axis=0)
        beside = beside + jnp.concatenate([v_ref[own:, at], jnp.where(is_even, even, odd)], axis=0)
        beside = beside + pltpu.roll(v, 1, 1) + pltpu.roll(v, cols - 1, 1)
        local = jnp.concatenate(
            [
                jnp.broadcast_to(stat[natoms + z : natoms + z + 1, inside : inside + cols], (own, cols))
                for z in range(planes)
            ],
            axis=0,
        )
        emit(at, (local + shift) * v - kinetic_scale * beside + nonlocal_term)


def gram_body(where_ref, mine_ref, other_ref, stat_m, stat_o, out_ref, *, own, planes, natoms):
    half = stat_m.shape[1]
    total = mine_ref.shape[0]
    span, quarter = total // 2, total // 4
    rows = pl.ds(pl.multiple_of(where_ref[1] * span, span), span)
    start = pl.multiple_of(where_ref[0], own)
    sums = jnp.zeros((span + own, total), f32)
    for orb_ref, stat in ((mine_ref, stat_m), (other_ref, stat_o)):
        for z in range(planes):
            at = slice(z * half, (z + 1) * half)
            source = stat[natoms + planes + z : natoms + planes + z + 1, :] * orb_ref[pl.ds(start, own), at]
            sums = sums + dot_nt(jnp.concatenate([orb_ref[rows, at], source], axis=0), orb_ref[:, at], three_passes)
    gram, corr = sums[0:span], sums[span:]
    twice = jnp.concatenate([gram, gram], axis=1)
    ahead = jnp.where(where_ref[1] == 0, twice[:, 0:total], twice[:, span : span + total])
    out_ref[...] = jnp.concatenate(
        [
            ahead[0:quarter, 0 : 3 * quarter],
            ahead[quarter:, quarter:],
            jnp.concatenate([corr[:, 0:span], corr[:, span:]], axis=0),
        ],
        axis=1,
    )


def gram_from(low, high):
    quarter = low.shape[0]
    blocks = [
        [part[:, i + d * quarter : i + (d + 1) * quarter] * (1.0 if d == 1 else 0.5) for d in range(3)]
        + [jnp.zeros((quarter, quarter), f32)]
        for part in (low, high)
        for i in (0, 3 * quarter)
    ]
    upper = jnp.concatenate(
        [jnp.concatenate([blocks[j][(k - j) % 4] for k in range(4)], axis=1) for j in range(4)], axis=0
    )
    return upper + upper.T


def inverse_of(gram):
    n = gram.shape[0]
    eye = (lax.broadcasted_iota(jnp.int32, (n, n), 0) == lax.broadcasted_iota(jnp.int32, (n, n), 1)).astype(f32)
    work = jnp.concatenate([gram, eye], axis=1)
    tiles = [work[i : i + 8] for i in range(0, n, 8)]
    sub = lax.broadcasted_iota(jnp.int32, (8, 2 * n), 0)
    for k in range(0, n, 2):
        t, r = divmod(k, 8)
        row0, row1 = tiles[t][r : r + 1, :], tiles[t][r + 1 : r + 2, :]
        a, b, d = row0[:, k : k + 1], row0[:, k + 1 : k + 2], row1[:, k + 1 : k + 2]
        det = a * d - b * b
        over = 1.0 / det
        x0 = row0 * (d * over) - row1 * (b * over)
        x1 = row1 * (a * over) - row0 * (b * over)
        for i in range(t, n // 8):
            step = tiles[i] - tiles[i][:, k : k + 1] * x0 - tiles[i][:, k + 1 : k + 2] * x1
            if i == t:
                first = row0 * lax.rsqrt(a)
                second = (row1 - row0 * (b / a)) * lax.rsqrt(det / a)
                kept = jnp.where(sub == r, first, jnp.where(sub == r + 1, second, tiles[i]))
                step = jnp.where(sub > r + 1, step, kept)
            tiles[i] = step
    lower_inverse = jnp.concatenate(tiles, axis=0)[:, n:]
    inv = lax.dot_general(
        lower_inverse, lower_inverse, (((0,), (0,)), ((), ())), precision=highest, preferred_element_type=f32
    )
    return 2.0 * inv - dot_nn(dot_nn(inv, gram), inv)


def source_body(
    where_ref, sums_ref, swapped_ref, mine_hbm, other_hbm, stat_m, stat_o, w_ref,
    r_ref, even_edge, odd_edge, pc_ref, inv_ref, own_ref, mine_ref, other_ref, sems, *, own, planes, natoms, cells,
):
    arriving = copies([(mine_hbm, mine_ref), (other_hbm, other_ref)], sems)
    for copy in arriving:
        copy.start()
    half = stat_m.shape[1]
    total = mine_ref.shape[0]
    ours, theirs = sums_ref[...], swapped_ref[...]
    first = where_ref[1] == 0
    gram = gram_from(jnp.where(first, ours, theirs), jnp.where(first, theirs, ours)) / cells
    inv = inverse_of(gram)
    inv_ref[...] = inv
    folded = ours[:, 2 * total - total // 2 :] / cells
    g = dot_nn(jnp.concatenate([folded[0:own], folded[own:]], axis=1), inv)
    start = pl.multiple_of(where_ref[0], own)
    for copy in arriving:
        copy.wait()
    for h, (orb_ref, stat) in enumerate(((mine_ref, stat_m), (other_ref, stat_o))):
        for z in range(planes):
            at = slice(z * half, (z + 1) * half)
            mine = orb_ref[pl.ds(start, own), at]
            source = stat[natoms + planes + z : natoms + planes + z + 1, :] * mine
            own_ref[z * own : (z + 1) * own, h * half : (h + 1) * half] = mine
            r_ref[z * own : (z + 1) * own, h * half : (h + 1) * half] = dot_nn(g, orb_ref[:, at]) - source
    pc = inner_partials(r_ref, (stat_m, stat_o), w_ref, own, natoms)
    pc_ref[...] = pc
    pack_edges(w_ref, r_ref, pc, even_edge, odd_edge, own)


def first_body(
    v_ref, pc_ref, odd_ref, even_ref, stat_m, stat_o, w_ref, en_ref,
    f_ref, even_edge, odd_edge, out_pc_ref, *, own, natoms, cols,
):
    def emit(at, block):
        f_ref[:, at] = block

    apply_shift(emit, v_ref, pc_ref, odd_ref, even_ref, (stat_m, stat_o), w_ref, en_ref, cols)
    pc = inner_partials(f_ref, (stat_m, stat_o), w_ref, own, natoms)
    out_pc_ref[...] = pc
    pack_edges(w_ref, f_ref, pc, even_edge, odd_edge, own)


def target_body(
    v_ref, pc_ref, odd_ref, even_ref, stat_m, stat_o, w_ref, en_ref, r_ref, mine_hbm, other_hbm,
    t_ref, out_ref, mine_ref, other_ref, sems, *, own, planes, cols,
):
    arriving = copies([(mine_hbm, mine_ref), (other_hbm, other_ref)], sems)
    for copy in arriving:
        copy.start()
    square = squared_frequency(w_ref)

    def emit(at, block):
        t_ref[:, at] = block + square * r_ref[:, at]

    apply_shift(emit, v_ref, pc_ref, odd_ref, even_ref, (stat_m, stat_o), w_ref, en_ref, cols)
    half = stat_m.shape[1]
    total = mine_ref.shape[0]
    corr = jnp.zeros((own, total), f32)
    for copy in arriving:
        copy.wait()
    for h, orb_ref in enumerate((mine_ref, other_ref)):
        for z in range(planes):
            block = t_ref[z * own : (z + 1) * own, h * half : (h + 1) * half]
            corr = corr + dot_nt(block, orb_ref[:, z * half : (z + 1) * half], three_passes)
    rr = orbital_row_sums([b * b for b in lane_blocks(r_ref, cols)], own)
    ff = orbital_row_sums([b * b for b in lane_blocks(v_ref, cols)], own)
    lanes = out_ref.shape[1]
    lane = lax.broadcasted_iota(jnp.int32, (own, lanes), 1)
    spread = jnp.concatenate([corr, jnp.zeros((own, lanes - total), f32)], axis=1)
    out_ref[...] = jnp.where(lane == total, rr, jnp.where(lane == total + 1, ff, spread))


def residual_body(
    sums_ref, inv_ref, r_ref, t_ref, mine_ref, other_ref, stat_m, stat_o, w_ref,
    out_ref, even_edge, odd_edge, pc_ref, *, own, planes, natoms, cells,
):
    half = stat_m.shape[1]
    total = mine_ref.shape[0]
    square = squared_frequency(w_ref)
    g = dot_nn(sums_ref[:, 0:total] / cells, inv_ref[...])
    rr, ff = sums_ref[:, total : total + 1], sums_ref[:, total + 1 : total + 2]
    step = rr / (ff + square * rr)
    for h, orb_ref in enumerate((mine_ref, other_ref)):
        for z in range(planes):
            rows, at = slice(z * own, (z + 1) * own), slice(h * half, (h + 1) * half)
            image = t_ref[rows, at] - dot_nn(g, orb_ref[:, z * half : (z + 1) * half])
            out_ref[rows, at] = r_ref[rows, at] - step * image
    pc = inner_partials(out_ref, (stat_m, stat_o), w_ref, own, natoms)
    pc_ref[...] = pc
    pack_edges(w_ref, out_ref, pc, even_edge, odd_edge, own)


def last_body(
    v_ref, pc_ref, odd_ref, even_ref, stat_m, stat_o, w_ref, en_ref, r_ref, f_ref, u_ref, out_ref, *, own, cols
):
    def emit(at, block):
        u_ref[:, at] = block

    apply_shift(emit, v_ref, pc_ref, odd_ref, even_ref, (stat_m, stat_o), w_ref, en_ref, cols)
    r1, r0, u1, u0 = (lane_blocks(ref, cols) for ref in (v_ref, r_ref, u_ref, f_ref))
    values = [
        orbital_row_sums([a * b for a, b in zip(x, y)], own) for x, y in ((r1, r1), (u1, u1), (u1, u0), (r1, r0))
    ]
    lanes = out_ref.shape[1]
    lane = lax.broadcasted_iota(jnp.int32, (own, lanes), 1)
    row = lax.broadcasted_iota(jnp.int32, (own, lanes), 0)
    placed = sum(jnp.where(lane == own * s + row, value, 0.0) for s, value in enumerate(values))
    out_ref[...] = jnp.sum(placed, axis=0, keepdims=True)


def response_body(
    sums_ref, lines_ref, f_ref, u_ref, own_ref, w_ref, out_ref, swap_ref, dens_ref, *, own, planes
):
    total = sums_ref.shape[1] // 2
    half = f_ref.shape[1] // 2
    square = squared_frequency(w_ref)
    rr0, ff = sums_ref[:, total : total + 1], sums_ref[:, total + 1 : total + 2]
    line = lines_ref[...]
    lanes = line.shape[1]
    lane = lax.broadcasted_iota(jnp.int32, (own, lanes), 1)
    row = lax.broadcasted_iota(jnp.int32, (own, lanes), 0)
    rr1, uu, uf, rx = (
        jnp.sum(jnp.where(lane == own * s + row, line, 0.0), axis=1, keepdims=True) for s in range(4)
    )
    step0 = rr0 / (ff + square * rr0)
    beta = rr1 / rr0
    curvature = uu + 2.0 * beta * uf + beta * beta * ff + square * (rr1 + 2.0 * beta * rx + beta * beta * rr0)
    step1 = rr1 / curvature
    swap_ref[own:, :] = jnp.zeros((swap_ref.shape[0] - own, swap_ref.shape[1]), f32)
    for h in range(2):
        for z in range(planes):
            rows, at = slice(z * own, (z + 1) * own), slice(h * half, (h + 1) * half)
            to = slice(z * half, (z + 1) * half)
            response = (step0 + step1 * beta) * f_ref[rows, at] + step1 * u_ref[rows, at]
            dens = jnp.sum(own_ref[rows, at] * response, axis=0, keepdims=True)
            if h == 0:
                out_ref[:, to] = response
                dens_ref[:, to] = dens
            else:
                swap_ref[0:own, to] = response
                swap_ref[own : own + 1, to] = dens


def copy_for_each(array, axis):
    copies = jnp.broadcast_to(array, (lax.axis_size(axis), *array.shape))
    return lax.all_to_all(copies, axis, split_axis=0, concat_axis=0, tiled=True)


def swap_cores(array):
    return lax.ppermute(array, "pen", [(0, 1), (1, 0)])


def turn(slab):
    return (slab + slab // NEAR) % 2


def place(slab, part):
    return 2 * slab + (part + turn(slab)) % 2


def summed(array):
    count = lax.axis_size("slab")
    runs = [[place(i + j, part) for j in range(NEAR)] for part in range(2) for i in range(0, count, NEAR)]
    across = [[place(i + j, part) for i in range(0, count, NEAR)] for part in range(2) for j in range(NEAR)]
    array = lax.psum(array, ("slab", "pen"), axis_index_groups=runs)
    return lax.psum(array, ("slab", "pen"), axis_index_groups=across)


def from_neighbours(even_edge, odd_edge):
    count = lax.axis_size("slab")

    def pairs(first):
        both = [(i, (i + 1) % count) for i in range(first, count, 2)]
        return [(place(a, part), place(b, part)) for i, j in both for a, b in ((i, j), (j, i)) for part in range(2)]

    axes = ("slab", "pen")
    return lax.ppermute(odd_edge, axes, pairs(1)), lax.ppermute(even_edge, axes, pairs(0))


def plane_weights(atom_planes, profiles, planes, depth_total):
    span_size = profiles.shape[1]
    covered = (atom_planes[:, None] + jnp.arange(span_size, dtype=jnp.int32)[None, :]) % depth_total
    matches = (covered[None, :, :] == planes[:, None, None]).astype(jnp.float32)
    return jnp.sum(profiles[None, :, :] * matches, axis=2)


def on_device(
    orbitals, energies, frequency, local_potential, perturbation, projectors, profiles, couplings, atom_planes
):
    chip_count, planes, row_count, cols = orbitals.shape
    natoms = projectors.shape[0]
    half = row_count * cols
    slabs = lax.axis_size("slab")
    assert lax.axis_size("pen") == 2 and slabs > 2 and slabs % 2 == 0
    assert profiles.shape[1] == planes + 1
    depth_total = planes * slabs
    cells = float(depth_total * 2 * half)
    own = chip_count // 2
    slab = lax.axis_index("slab")
    core = (lax.axis_index("pen") + turn(slab)) % 2
    crossings = [(turn(slab) + turn((slab + step) % slabs)) % 2 for step in (1, slabs - 1)]
    first_plane = slab * planes
    weights = plane_weights(atom_planes, profiles, first_plane + jnp.arange(planes, dtype=jnp.int32), depth_total)
    where = jnp.stack([lax.axis_index("orb") * chip_count + core * own, core]).astype(jnp.int32)
    own_energies = lax.dynamic_slice(energies, (core * own,), (own,)).reshape(own, 1)
    up_even = slab % 2 == 0
    flags = [up_even, jnp.where(up_even, *crossings), jnp.where(up_even, *crossings[::-1])]
    below = jnp.stack([frequency[0] * frequency[0], *(f.astype(f32) for f in flags)])
    weights = jnp.concatenate(
        [weights, couplings.reshape(1, natoms), jnp.broadcast_to(below[:, None], (BELOW - 1, natoms))], axis=0
    )

    stat_m = jnp.concatenate(
        [a.reshape(-1, half) for a in (projectors, local_potential, perturbation)], axis=0
    )
    stat_o = swap_cores(stat_m)
    mine = copy_for_each(orbitals.reshape(chip_count, planes * half), "orb").reshape(-1, planes * half)
    other = swap_cores(mine)
    total = mine.shape[0]
    stats = (stat_m, stat_o)
    field, edge, part = (planes * own, 2 * half), (own, 2 * half + natoms), (own, natoms)

    (gram_part,) = call(
        functools.partial(gram_body, own=own, planes=planes, natoms=natoms),
        (where, mine, other, *stats), "svvkk", [(total // 4, 2 * total)],
    )
    gram_sum = summed(gram_part)
    gram_other = swap_cores(gram_sum)
    r0, even, odd, pc, inv, own_orbitals = call(
        functools.partial(source_body, own=own, planes=planes, natoms=natoms, cells=cells),
        (where, gram_sum, gram_other, mine, other, *stats, weights), "skkhhkkk",
        [field, edge, edge, part, (total, total), field],
    )
    odd, even = from_neighbours(even, odd)
    first, even, odd, first_pc = call(
        functools.partial(first_body, own=own, natoms=natoms, cols=cols),
        (r0, pc, odd, even, *stats, weights, own_energies), "kkkkkkkk", [field, edge, edge, part],
    )
    odd, even = from_neighbours(even, odd)
    target, sums_part = call(
        functools.partial(target_body, own=own, planes=planes, cols=cols),
        (first, first_pc, odd, even, *stats, weights, own_energies, r0, mine, other), "kkkkkkkkkhh",
        [field, (own, 2 * total)],
    )
    sums = summed(sums_part)
    r1, even, odd, pc = call(
        functools.partial(residual_body, own=own, planes=planes, natoms=natoms, cells=cells),
        (sums, inv, r0, target, mine, other, *stats, weights), "kkkkvvkkk", [field, edge, edge, part],
    )
    odd, even = from_neighbours(even, odd)
    last, lines = call(
        functools.partial(last_body, own=own, cols=cols),
        (r1, pc, odd, even, *stats, weights, own_energies, r0, first), "kkkkkkkkkk",
        [field, (1, 2 * total)],
    )
    lines = summed(lines)
    response, to_other, dens = call(
        functools.partial(response_body, own=own, planes=planes),
        (sums, lines, first, last, own_orbitals, weights), "kkkkkk",
        [(own, planes * half), (2 * own, planes * half), (1, planes * half)],
    )
    got = swap_cores(to_other)
    theirs = got[0:own]
    low, high = jnp.where(core == 0, response, theirs), jnp.where(core == 0, theirs, response)
    response_real = jnp.concatenate([low, high], axis=0).reshape(orbitals.shape)
    dens = (dens + got[own : own + 1]).reshape(planes, half)
    density = copy_for_each(dens, "orb").sum(axis=0) * (4.0 / NOCC)
    return response_real, density.reshape(planes, row_count, cols)


def solution(mesh):
    in_specs = (
        P(("parts", "orb"), "slab", "pen", None),
        P(("parts", "orb")),
        P("parts"),
        P("slab", "pen", None),
        P("slab", "pen", None),
        P(None, "pen", None),
        P(),
        P(),
        P(),
    )
    out_specs = (P(("parts", "orb"), "slab", "pen", None), P(("parts", "slab"), "pen", None))
    return jax.shard_map(on_device, mesh=mesh, in_specs=in_specs, out_specs=out_specs, check_vma=False)
```

```python
import functools

import jax
import jax.numpy as jnp
from jax import lax
from jax.experimental import pallas as pl
from jax.experimental.pallas import tpu as pltpu
from jax.sharding import PartitionSpec as P

NOCC = 64
NEAR = 4

kinetic_scale = 0.125
highest, three_passes = lax.Precision.HIGHEST, lax.Precision.HIGH
f32 = jnp.float32
VMEM = pl.BlockSpec(memory_space=pltpu.VMEM)
SMEM = pl.BlockSpec(memory_space=pltpu.SMEM)


def dot_nn(a, b, precision=highest):
    return lax.dot_general(a, b, (((1,), (0,)), ((), ())), precision=precision, preferred_element_type=f32)


def dot_nt(a, b, precision=highest):
    return lax.dot_general(a, b, (((1,), (1,)), ((), ())), precision=precision, preferred_element_type=f32)


def call(body, args, kinds, outs, last_in_hbm=False):
    late = [pltpu.VMEM(a.shape, f32) for a, k in zip(args, kinds, strict=True) if k == "h"]
    args = [pltpu.with_memory_space_constraint(a, pltpu.VMEM) if k == "k" else a for a, k in zip(args, kinds, strict=True)]
    return pl.pallas_call(
        body,
        in_specs=[SMEM if k == "s" else pl.BlockSpec(memory_space=pl.ANY) if k == "h" else VMEM for k in kinds],
        out_specs=[VMEM] * len(outs),
        out_shape=[
            jax.ShapeDtypeStruct(s, f32) if last_in_hbm and i == len(outs) - 1 else pltpu.VMEM(s, f32)
            for i, s in enumerate(outs)
        ],
        scratch_shapes=[*late, pltpu.SemaphoreType.DMA((len(late),))] if late else [],
    )(*args)


def copies(pairs, sems):
    return [pltpu.make_async_copy(a, b, sems.at[i]) for i, (a, b) in enumerate(pairs)]


BELOW = 5


def flag(w_ref, row, shape):
    at = w_ref.shape[0] - BELOW + row
    return jnp.broadcast_to(w_ref[at : at + 1, 0:1], shape) > 0.5


def squared_frequency(w_ref):
    at = w_ref.shape[0] - BELOW + 1
    return w_ref[at : at + 1, 0:1]


def orbital_row_sums(products, own):
    total = functools.reduce(jnp.add, products)
    folded = functools.reduce(jnp.add, [total[i : i + own] for i in range(0, total.shape[0], own)])
    return jnp.sum(folded, axis=1, keepdims=True)


def lane_blocks(ref, cols):
    return [ref[:, i : i + cols] for i in range(0, ref.shape[1], cols)]


def inner_partials(v_ref, stat_refs, w_ref, own, natoms):
    half = stat_refs[0].shape[1]
    sums = sum(
        dot_nt(v_ref[:, h * half : (h + 1) * half], stat_refs[h][0:natoms, :], three_passes) for h in range(2)
    )
    planes = w_ref.shape[0] - BELOW
    return sum(sums[z * own : (z + 1) * own] * w_ref[z : z + 1, :] for z in range(planes))


def pack_edges(w_ref, v_ref, pc, even_ref, odd_ref, own):
    width = v_ref.shape[1]
    half = width // 2
    is_even = flag(w_ref, 2, (own, width))
    top, bottom = v_ref[v_ref.shape[0] - own :, :], v_ref[0:own, :]
    for ref, edge, row in ((even_ref, jnp.where(is_even, top, bottom), 3), (odd_ref, jnp.where(is_even, bottom, top), 4)):
        crossing = flag(w_ref, row, (own, half))
        ref[:, 0:half] = jnp.where(crossing, edge[:, half:], edge[:, 0:half])
        ref[:, half:width] = jnp.where(crossing, edge[:, 0:half], edge[:, half:])
        ref[:, width:] = pc


def apply_shift(emit, v_ref, pc_ref, odd_ref, even_ref, stat_refs, w_ref, en_ref, cols):
    own = odd_ref.shape[0]
    is_even = flag(w_ref, 2, (own, cols))
    planes, natoms = w_ref.shape[0] - BELOW, w_ref.shape[1]
    width = v_ref.shape[1]
    half = width // 2
    c = w_ref[planes : planes + 1, :] * (pc_ref[...] + odd_ref[:, width:] + even_ref[:, width:])
    spread = jnp.concatenate([c * w_ref[z : z + 1, :] for z in range(planes)], axis=0)
    shift = jnp.concatenate([6.0 * kinetic_scale - en_ref[...]] * planes, axis=0)
    blocks = width // cols
    for k in range(blocks):
        at = slice(k * cols, (k + 1) * cols)
        stat = stat_refs[k * cols // half]
        inside = (k * cols) % half
        odd, even = odd_ref[:, at], even_ref[:, at]
        nonlocal_term = dot_nn(spread, stat[0:natoms, inside : inside + cols], three_passes)
        v = v_ref[:, at]
        after, before = (k + 1) % blocks, (k - 1) % blocks
        beside = v_ref[:, after * cols : (after + 1) * cols] + v_ref[:, before * cols : (before + 1) * cols]
        beside = beside + jnp.concatenate([jnp.where(is_even, odd, even), v_ref[0 : own * (planes - 1), at]], axis=0)
        beside = beside + jnp.concatenate([v_ref[own:, at], jnp.where(is_even, even, odd)], axis=0)
        beside = beside + pltpu.roll(v, 1, 1) + pltpu.roll(v, cols - 1, 1)
        local = jnp.concatenate(
            [
                jnp.broadcast_to(stat[natoms + z : natoms + z + 1, inside : inside + cols], (own, cols))
                for z in range(planes)
            ],
            axis=0,
        )
        emit(at, (local + shift) * v - kinetic_scale * beside + nonlocal_term)


def gram_body(where_ref, mine_ref, other_ref, stat_m, stat_o, out_ref, *, own, planes, natoms):
    half = stat_m.shape[1]
    total = mine_ref.shape[0]
    span, quarter = total // 2, total // 4
    rows = pl.ds(pl.multiple_of(where_ref[1] * span, span), span)
    start = pl.multiple_of(where_ref[0], own)
    sums = jnp.zeros((span + own, total), f32)
    for orb_ref, stat in ((mine_ref, stat_m), (other_ref, stat_o)):
        for z in range(planes):
            at = slice(z * half, (z + 1) * half)
            source = stat[natoms + planes + z : natoms + planes + z + 1, :] * orb_ref[pl.ds(start, own), at]
            sums = sums + dot_nt(jnp.concatenate([orb_ref[rows, at], source], axis=0), orb_ref[:, at], three_passes)
    gram, corr = sums[0:span], sums[span:]
    twice = jnp.concatenate([gram, gram], axis=1)
    ahead = jnp.where(where_ref[1] == 0, twice[:, 0:total], twice[:, span : span + total])
    out_ref[...] = jnp.concatenate(
        [
            ahead[0:quarter, 0 : 3 * quarter],
            ahead[quarter:, quarter:],
            jnp.concatenate([corr[:, 0:span], corr[:, span:]], axis=0),
        ],
        axis=1,
    )


def gram_from(low, high):
    quarter = low.shape[0]
    blocks = [
        [part[:, i + d * quarter : i + (d + 1) * quarter] * (1.0 if d == 1 else 0.5) for d in range(3)]
        + [jnp.zeros((quarter, quarter), f32)]
        for part in (low, high)
        for i in (0, 3 * quarter)
    ]
    upper = jnp.concatenate(
        [jnp.concatenate([blocks[j][(k - j) % 4] for k in range(4)], axis=1) for j in range(4)], axis=0
    )
    return upper + upper.T


def inverse_of(gram):
    n = gram.shape[0]
    eye = (lax.broadcasted_iota(jnp.int32, (n, n), 0) == lax.broadcasted_iota(jnp.int32, (n, n), 1)).astype(f32)
    work = jnp.concatenate([gram, eye], axis=1)
    tiles = [work[i : i + 8] for i in range(0, n, 8)]
    sub = lax.broadcasted_iota(jnp.int32, (8, 2 * n), 0)
    for k in range(0, n, 2):
        t, r = divmod(k, 8)
        row0, row1 = tiles[t][r : r + 1, :], tiles[t][r + 1 : r + 2, :]
        a, b, d = row0[:, k : k + 1], row0[:, k + 1 : k + 2], row1[:, k + 1 : k + 2]
        det = a * d - b * b
        over = 1.0 / det
        x0 = row0 * (d * over) - row1 * (b * over)
        x1 = row1 * (a * over) - row0 * (b * over)
        for i in range(t, n // 8):
            step = tiles[i] - tiles[i][:, k : k + 1] * x0 - tiles[i][:, k + 1 : k + 2] * x1
            if i == t:
                first = row0 * lax.rsqrt(a)
                second = (row1 - row0 * (b / a)) * lax.rsqrt(det / a)
                kept = jnp.where(sub == r, first, jnp.where(sub == r + 1, second, tiles[i]))
                step = jnp.where(sub > r + 1, step, kept)
            tiles[i] = step
    lower_inverse = jnp.concatenate(tiles, axis=0)[:, n:]
    inv = lax.dot_general(
        lower_inverse, lower_inverse, (((0,), (0,)), ((), ())), precision=highest, preferred_element_type=f32
    )
    return 2.0 * inv - dot_nn(dot_nn(inv, gram), inv)


def source_body(
    where_ref, sums_ref, swapped_ref, mine_hbm, other_hbm, stat_m, stat_o, w_ref,
    r_ref, even_edge, odd_edge, pc_ref, inv_ref, own_ref, mine_ref, other_ref, sems, *, own, planes, natoms, cells,
):
    arriving = copies([(mine_hbm, mine_ref), (other_hbm, other_ref)], sems)
    for copy in arriving:
        copy.start()
    half = stat_m.shape[1]
    total = mine_ref.shape[0]
    ours, theirs = sums_ref[...], swapped_ref[...]
    first = where_ref[1] == 0
    gram = gram_from(jnp.where(first, ours, theirs), jnp.where(first, theirs, ours)) / cells
    inv = inverse_of(gram)
    inv_ref[...] = inv
    folded = ours[:, 2 * total - total // 2 :] / cells
    g = dot_nn(jnp.concatenate([folded[0:own], folded[own:]], axis=1), inv)
    start = pl.multiple_of(where_ref[0], own)
    for copy in arriving:
        copy.wait()
    for h, (orb_ref, stat) in enumerate(((mine_ref, stat_m), (other_ref, stat_o))):
        for z in range(planes):
            at = slice(z * half, (z + 1) * half)
            mine = orb_ref[pl.ds(start, own), at]
            source = stat[natoms + planes + z : natoms + planes + z + 1, :] * mine
            own_ref[z * own : (z + 1) * own, h * half : (h + 1) * half] = mine
            r_ref[z * own : (z + 1) * own, h * half : (h + 1) * half] = dot_nn(g, orb_ref[:, at]) - source
    pc = inner_partials(r_ref, (stat_m, stat_o), w_ref, own, natoms)
    pc_ref[...] = pc
    pack_edges(w_ref, r_ref, pc, even_edge, odd_edge, own)


def first_body(
    v_ref, pc_ref, odd_ref, even_ref, stat_m, stat_o, w_ref, en_ref,
    f_ref, even_edge, odd_edge, out_pc_ref, *, own, natoms, cols,
):
    def emit(at, block):
        f_ref[:, at] = block

    apply_shift(emit, v_ref, pc_ref, odd_ref, even_ref, (stat_m, stat_o), w_ref, en_ref, cols)
    pc = inner_partials(f_ref, (stat_m, stat_o), w_ref, own, natoms)
    out_pc_ref[...] = pc
    pack_edges(w_ref, f_ref, pc, even_edge, odd_edge, own)


def target_body(
    v_ref, pc_ref, odd_ref, even_ref, stat_m, stat_o, w_ref, en_ref, r_ref, mine_hbm, other_hbm,
    t_ref, out_ref, mine_ref, other_ref, sems, *, own, planes, cols,
):
    arriving = copies([(mine_hbm, mine_ref), (other_hbm, other_ref)], sems)
    for copy in arriving:
        copy.start()
    square = squared_frequency(w_ref)

    def emit(at, block):
        t_ref[:, at] = block + square * r_ref[:, at]

    apply_shift(emit, v_ref, pc_ref, odd_ref, even_ref, (stat_m, stat_o), w_ref, en_ref, cols)
    half = stat_m.shape[1]
    total = mine_ref.shape[0]
    corr = jnp.zeros((own, total), f32)
    for copy in arriving:
        copy.wait()
    for h, orb_ref in enumerate((mine_ref, other_ref)):
        for z in range(planes):
            block = t_ref[z * own : (z + 1) * own, h * half : (h + 1) * half]
            corr = corr + dot_nt(block, orb_ref[:, z * half : (z + 1) * half], three_passes)
    rr = orbital_row_sums([b * b for b in lane_blocks(r_ref, cols)], own)
    ff = orbital_row_sums([b * b for b in lane_blocks(v_ref, cols)], own)
    lanes = out_ref.shape[1]
    lane = lax.broadcasted_iota(jnp.int32, (own, lanes), 1)
    spread = jnp.concatenate([corr, jnp.zeros((own, lanes - total), f32)], axis=1)
    out_ref[...] = jnp.where(lane == total, rr, jnp.where(lane == total + 1, ff, spread))


def residual_body(
    sums_ref, inv_ref, r_ref, t_ref, mine_ref, other_ref, stat_m, stat_o, w_ref,
    out_ref, even_edge, odd_edge, pc_ref, *, own, planes, natoms, cells,
):
    half = stat_m.shape[1]
    total = mine_ref.shape[0]
    square = squared_frequency(w_ref)
    g = dot_nn(sums_ref[:, 0:total] / cells, inv_ref[...])
    rr, ff = sums_ref[:, total : total + 1], sums_ref[:, total + 1 : total + 2]
    step = rr / (ff + square * rr)
    for h, orb_ref in enumerate((mine_ref, other_ref)):
        for z in range(planes):
            rows, at = slice(z * own, (z + 1) * own), slice(h * half, (h + 1) * half)
            image = t_ref[rows, at] - dot_nn(g, orb_ref[:, z * half : (z + 1) * half])
            out_ref[rows, at] = r_ref[rows, at] - step * image
    pc = inner_partials(out_ref, (stat_m, stat_o), w_ref, own, natoms)
    pc_ref[...] = pc
    pack_edges(w_ref, out_ref, pc, even_edge, odd_edge, own)


def last_body(
    v_ref, pc_ref, odd_ref, even_ref, stat_m, stat_o, w_ref, en_ref, r_ref, f_ref, u_ref, out_ref, *, own, cols
):
    def emit(at, block):
        u_ref[:, at] = block

    apply_shift(emit, v_ref, pc_ref, odd_ref, even_ref, (stat_m, stat_o), w_ref, en_ref, cols)
    r1, r0, u1, u0 = (lane_blocks(ref, cols) for ref in (v_ref, r_ref, u_ref, f_ref))
    values = [
        orbital_row_sums([a * b for a, b in zip(x, y)], own) for x, y in ((r1, r1), (u1, u1), (u1, u0), (r1, r0))
    ]
    lanes = out_ref.shape[1]
    lane = lax.broadcasted_iota(jnp.int32, (own, lanes), 1)
    row = lax.broadcasted_iota(jnp.int32, (own, lanes), 0)
    placed = sum(jnp.where(lane == own * s + row, value, 0.0) for s, value in enumerate(values))
    out_ref[...] = jnp.sum(placed, axis=0, keepdims=True)


def response_body(
    sums_ref, lines_ref, f_ref, u_ref, own_ref, w_ref, out_ref, swap_ref, dens_ref, *, own, planes
):
    total = sums_ref.shape[1] // 2
    half = f_ref.shape[1] // 2
    square = squared_frequency(w_ref)
    rr0, ff = sums_ref[:, total : total + 1], sums_ref[:, total + 1 : total + 2]
    line = lines_ref[...]
    lanes = line.shape[1]
    lane = lax.broadcasted_iota(jnp.int32, (own, lanes), 1)
    row = lax.broadcasted_iota(jnp.int32, (own, lanes), 0)
    rr1, uu, uf, rx = (
        jnp.sum(jnp.where(lane == own * s + row, line, 0.0), axis=1, keepdims=True) for s in range(4)
    )
    step0 = rr0 / (ff + square * rr0)
    beta = rr1 / rr0
    curvature = uu + 2.0 * beta * uf + beta * beta * ff + square * (rr1 + 2.0 * beta * rx + beta * beta * rr0)
    step1 = rr1 / curvature
    swap_ref[own:, :] = jnp.zeros((swap_ref.shape[0] - own, swap_ref.shape[1]), f32)
    for h in range(2):
        for z in range(planes):
            rows, at = slice(z * own, (z + 1) * own), slice(h * half, (h + 1) * half)
            to = slice(z * half, (z + 1) * half)
            response = (step0 + step1 * beta) * f_ref[rows, at] + step1 * u_ref[rows, at]
            dens = jnp.sum(own_ref[rows, at] * response, axis=0, keepdims=True)
            if h == 0:
                out_ref[:, to] = response
                dens_ref[:, to] = dens
            else:
                swap_ref[0:own, to] = response
                swap_ref[own : own + 1, to] = dens


def copy_for_each(array, axis):
    copies = jnp.broadcast_to(array, (lax.axis_size(axis), *array.shape))
    return lax.all_to_all(copies, axis, split_axis=0, concat_axis=0, tiled=True)


def swap_cores(array):
    return lax.ppermute(array, "pen", [(0, 1), (1, 0)])


def turn(slab):
    return (slab + slab // NEAR) % 2


def place(slab, part):
    return 2 * slab + (part + turn(slab)) % 2


def summed(array):
    count = lax.axis_size("slab")
    runs = [[place(i + j, part) for j in range(NEAR)] for part in range(2) for i in range(0, count, NEAR)]
    across = [[place(i + j, part) for i in range(0, count, NEAR)] for part in range(2) for j in range(NEAR)]
    array = lax.psum(array, ("slab", "pen"), axis_index_groups=runs)
    return lax.psum(array, ("slab", "pen"), axis_index_groups=across)


def from_neighbours(even_edge, odd_edge):
    count = lax.axis_size("slab")

    def pairs(first):
        both = [(i, (i + 1) % count) for i in range(first, count, 2)]
        return [(place(a, part), place(b, part)) for i, j in both for a, b in ((i, j), (j, i)) for part in range(2)]

    axes = ("slab", "pen")
    return lax.ppermute(odd_edge, axes, pairs(1)), lax.ppermute(even_edge, axes, pairs(0))


def plane_weights(atom_planes, profiles, planes, depth_total):
    span_size = profiles.shape[1]
    covered = (atom_planes[:, None] + jnp.arange(span_size, dtype=jnp.int32)[None, :]) % depth_total
    matches = (covered[None, :, :] == planes[:, None, None]).astype(jnp.float32)
    return jnp.sum(profiles[None, :, :] * matches, axis=2)


def on_device(
    orbitals, energies, frequency, local_potential, perturbation, projectors, profiles, couplings, atom_planes
):
    chip_count, planes, row_count, cols = orbitals.shape
    natoms = projectors.shape[0]
    half = row_count * cols
    slabs = lax.axis_size("slab")
    assert lax.axis_size("pen") == 2 and slabs > 2 and slabs % 2 == 0
    assert profiles.shape[1] == planes + 1
    depth_total = planes * slabs
    cells = float(depth_total * 2 * half)
    own = chip_count // 2
    slab = lax.axis_index("slab")
    core = (lax.axis_index("pen") + turn(slab)) % 2
    crossings = [(turn(slab) + turn((slab + step) % slabs)) % 2 for step in (1, slabs - 1)]
    first_plane = slab * planes
    weights = plane_weights(atom_planes, profiles, first_plane + jnp.arange(planes, dtype=jnp.int32), depth_total)
    where = jnp.stack([lax.axis_index("orb") * chip_count + core * own, core]).astype(jnp.int32)
    own_energies = lax.dynamic_slice(energies, (core * own,), (own,)).reshape(own, 1)
    up_even = slab % 2 == 0
    flags = [up_even, jnp.where(up_even, *crossings), jnp.where(up_even, *crossings[::-1])]
    below = jnp.stack([frequency[0] * frequency[0], *(f.astype(f32) for f in flags)])
    weights = jnp.concatenate(
        [weights, couplings.reshape(1, natoms), jnp.broadcast_to(below[:, None], (BELOW - 1, natoms))], axis=0
    )

    stat_m = jnp.concatenate(
        [a.reshape(-1, half) for a in (projectors, local_potential, perturbation)], axis=0
    )
    stat_o = swap_cores(stat_m)
    mine = copy_for_each(orbitals.reshape(chip_count, planes * half), "orb").reshape(-1, planes * half)
    other = swap_cores(mine)
    total = mine.shape[0]
    stats = (stat_m, stat_o)
    field, edge, part = (planes * own, 2 * half), (own, 2 * half + natoms), (own, natoms)

    (gram_part,) = call(
        functools.partial(gram_body, own=own, planes=planes, natoms=natoms),
        (where, mine, other, *stats), "svvkk", [(total // 4, 2 * total)],
    )
    gram_sum = summed(gram_part)
    gram_other = swap_cores(gram_sum)
    r0, even, odd, pc, inv, own_orbitals = call(
        functools.partial(source_body, own=own, planes=planes, natoms=natoms, cells=cells),
        (where, gram_sum, gram_other, mine, other, *stats, weights), "skkhhkkk",
        [field, edge, edge, part, (total, total), field], last_in_hbm=True,
    )
    odd, even = from_neighbours(even, odd)
    first, even, odd, first_pc = call(
        functools.partial(first_body, own=own, natoms=natoms, cols=cols),
        (r0, pc, odd, even, *stats, weights, own_energies), "kkkkkkkk", [field, edge, edge, part],
    )
    odd, even = from_neighbours(even, odd)
    target, sums_part = call(
        functools.partial(target_body, own=own, planes=planes, cols=cols),
        (first, first_pc, odd, even, *stats, weights, own_energies, r0, mine, other), "kkkkkkkkkhh",
        [field, (own, 2 * total)],
    )
    sums = summed(sums_part)
    r1, even, odd, pc = call(
        functools.partial(residual_body, own=own, planes=planes, natoms=natoms, cells=cells),
        (sums, inv, r0, target, mine, other, *stats, weights), "kkkkvvkkk", [field, edge, edge, part],
    )
    odd, even = from_neighbours(even, odd)
    last, lines = call(
        functools.partial(last_body, own=own, cols=cols),
        (r1, pc, odd, even, *stats, weights, own_energies, r0, first), "kkkkkkkkkk",
        [field, (1, 2 * total)],
    )
    lines = summed(lines)
    response, to_other, dens = call(
        functools.partial(response_body, own=own, planes=planes),
        (sums, lines, first, last, own_orbitals, weights), "kkkkvk",
        [(own, planes * half), (2 * own, planes * half), (1, planes * half)],
    )
    got = swap_cores(to_other)
    theirs = got[0:own]
    low, high = jnp.where(core == 0, response, theirs), jnp.where(core == 0, theirs, response)
    response_real = jnp.concatenate([low, high], axis=0).reshape(orbitals.shape)
    dens = (dens + got[own : own + 1]).reshape(planes, half)
    density = copy_for_each(dens, "orb").sum(axis=0) * (4.0 / NOCC)
    return response_real, density.reshape(planes, row_count, cols)


def solution(mesh):
    in_specs = (
        P(("parts", "orb"), "slab", "pen", None),
        P(("parts", "orb")),
        P("parts"),
        P("slab", "pen", None),
        P("slab", "pen", None),
        P(None, "pen", None),
        P(),
        P(),
        P(),
    )
    out_specs = (P(("parts", "orb"), "slab", "pen", None), P(("parts", "slab"), "pen", None))
    return jax.shard_map(on_device, mesh=mesh, in_specs=in_specs, out_specs=out_specs, check_vma=False)
```
